128 devices in a mesh: tm: 16 (over z, y_lo, core), member: 8 (over x, y_hi).
Axes of the slice: x: 4, y: 4 (y_hi: 2, y_lo: 2; y = y_hi * 2 + y_lo), z: 4, core: 2. Of those that a mesh axis runs over, the one named last changes fastest.
Arguments:
- fields: float32 [48, 96, 16384], P('member', 'tm'), may hold values from 200 to 350, as said below
Outputs:
- covariance: float32 [48, 48, 16384], P('member', None, 'tm')
The draws below stay inside these ranges and needn't reach their ends.
Inputs may be any that keep to these rules, and one draw needn't show every extreme that they name: `fields`: month t is calendar month t mod 12.
All inputs are finite; a program needn't handle non-finite values.
Results may differ from the reference program's by a relative error of at most 0.0003.
Values sent between devices are 32-bit elements; how exact they have to be, the bound alone decides.
A program may use at most 192 MiB of HBM per device.

```python
import math
import jax
import jax.numpy as jnp
from jax import lax

MEMBERS = 48
MONTHS = 96
PIXELS = 16384


def draw_fields(key, part):
    subkeys = jax.random.split(key, 7)
    offset = jax.random.uniform(subkeys[0], (1, 1, PIXELS), jnp.float32, 250.0, 300.0)
    amplitude = jnp.exp(jax.random.uniform(subkeys[1], (1, 1, PIXELS), jnp.float32, 0.0, math.log(20.0)))
    phase_shift = jax.random.uniform(subkeys[2], (1, 1, PIXELS), jnp.float32, 0.0, 12.0)
    pixel_scale = jnp.exp(jax.random.uniform(subkeys[3], (1, 1, PIXELS), jnp.float32, math.log(0.3), math.log(3.0)))
    weight = jax.random.uniform(subkeys[4], (1, 1, PIXELS), jnp.float32, 0.6, 1.2)
    calendar = (jnp.arange(MONTHS) % 12).astype(jnp.float32).reshape(1, MONTHS, 1)
    season = amplitude * jnp.sin(2.0 * math.pi * (calendar + phase_shift) / 12.0)
    common = jax.random.normal(subkeys[5], (1, MONTHS, PIXELS), jnp.float32)
    member_noise = jax.random.normal(subkeys[6], (MEMBERS, MONTHS, PIXELS), jnp.float32)
    member_scale = jnp.ones((MEMBERS, 1, 1), jnp.float32)
    values = offset + season + pixel_scale * member_scale * (weight * common + member_noise)
    return jnp.clip(values, 200.0, 350.0).astype(jnp.float32)


def setup_inputs(seed: int = 0) -> dict:
    keys = jax.random.split(jax.random.key(seed), 2)
    return {
        "fields": draw_fields(jax.random.fold_in(keys[1], 71), 0),
    }


def monthly_anomaly(series):
    members_here, months_here, pixel_count = series.shape
    by_year = series.reshape(members_here, months_here // 12, 12, pixel_count)
    climatology = jnp.mean(by_year, axis=1, keepdims=True)
    return (by_year - climatology).reshape(members_here, months_here, pixel_count)


def reference(fields):
    anomaly = monthly_anomaly(fields)
    products = jnp.einsum("itp,jtp->ijp", anomaly, anomaly, precision=lax.Precision.HIGHEST, preferred_element_type=jnp.float32)
    return products / (MONTHS - 12)
```

```python
import functools

import jax
import jax.numpy as jnp
from jax import lax
from jax.experimental import pallas as pl
from jax.experimental.pallas import tpu as pltpu
from jax.sharding import PartitionSpec as P

MESH = pl.DeviceIdType.MESH
F32 = jnp.float32
ORDER = ((2, 1), (2, 0), (1, 1), (3, 1), (1, 0), (3, 0), (0, 1), (0, 0))
LAST = len(ORDER) - 1


def contrasts(years):
    shifted = [y - years[0] for y in years[1:]]
    a1, a2, a3, a4, a5, a6, a7 = shifted
    p0, m0 = a4, -a4
    p1, m1 = a1 + a5, a1 - a5
    p2, m2 = a2 + a6, a2 - a6
    p3, m3 = a3 + a7, a3 - a7
    out = []
    q0, q2, q1, q3 = p0 + p2, p0 - p2, p1 + p3, p1 - p3
    out += [q0 - q1, q2 + q3, q2 - q3]
    r0, r2, r1, r3 = m0 + m2, m0 - m2, m1 + m3, m1 - m3
    out += [r0 + r1, r0 - r1, r2 + r3, r2 - r3]
    return out


def kernel(sizes, fields, out, raw, con, blk, got, send1, recv1, own, send3, recv3):
    tms, members, rows, mons, scale = sizes
    t, m = lax.axis_index("tm"), lax.axis_index("member")
    me = t * members + m
    total = tms * members
    x, h = m // 2, m % 2
    ten, low, core = t // 4, (t // 2) % 2, t % 2

    barrier = pltpu.get_barrier_semaphore()

    @pl.loop(1, total)
    def _(p):
        d = (me + p) % total
        pl.semaphore_signal(barrier, inc=1, device_id=(d // members, d % members), device_id_type=MESH)

    def pixels(d):
        return pl.ds(pl.multiple_of(d * 128, 128), 128)

    mine = pltpu.make_async_copy(fields.at[:, :, pixels(me)], raw.at[LAST * tms + t], own)
    mine.start()

    @pl.loop(0, con.shape[0])
    def _(s):
        con[s] = jnp.zeros(con.shape[1:], F32)

    pl.semaphore_wait(barrier, total - 1)

    for s, (dx, dh) in enumerate(ORDER):
        to_m = ((x + 4 - dx) % 4) * 2 + (h + dh) % 2

        @pl.loop(1 if s == LAST else 0, tms)
        def _(q, s=s, to_m=to_m):
            to_t = ((ten + q // 4) % 4) * 4 + ((low + (q // 2) % 2) % 2) * 2 + (core + q % 2) % 2
            pltpu.make_async_remote_copy(
                src_ref=fields.at[:, :, pixels(to_t * members + to_m)],
                dst_ref=raw.at[s * tms + t],
                send_sem=send1,
                recv_sem=recv1.at[s],
                device_id=(to_t, to_m),
                device_id_type=MESH,
            ).start()

    group = [((x + dx) % 4) * 2 + (h + dh) % 2 for dx, dh in ORDER]

    def transform(s):
        @pl.loop(0, rows)
        def _(i):
            for half in range(2):
                years = [raw[s * tms + 2 * y + half, i] for y in range(tms // 2)]
                for q, c in enumerate(contrasts(years)):
                    con[s, half * 7 + q, i, 0:mons] = c

    lane_row = lax.broadcasted_iota(jnp.int32, (8, 128), 0)

    def block(s, s2):
        cols = [jnp.zeros((8, 128), F32) for _ in range(rows)]
        for base in range(0, rows, 3):
            acc = [[None] * rows for _ in range(3)]
            for q in range(14):
                left = [con[s, q, base + a] for a in range(3)]
                right = [con[s2, q, b] for b in range(rows)]
                for a in range(3):
                    for b in range(rows):
                        prod = left[a] * right[b]
                        acc[a][b] = prod if q == 0 else acc[a][b] + prod
            for a in range(3):
                line = jnp.zeros((8, 128), F32)
                for b in range(rows):
                    r = jnp.sum(acc[a][b], axis=0, keepdims=True) * scale
                    r = jnp.broadcast_to(r, (8, 128))
                    line = jnp.where(lane_row == b, r, line)
                    cols[b] = jnp.where(lane_row == base + a, r, cols[b])
                blk[s, s2, base + a] = line[0:rows]
        for b in range(rows):
            blk[s2, s, b] = cols[b][0:rows]

    def ship(a, b):
        if a == LAST:
            return
        pltpu.make_async_remote_copy(
            src_ref=blk.at[a, b],
            dst_ref=got.at[m, group[b]],
            send_sem=send3,
            recv_sem=recv3,
            device_id=(t, group[a]),
            device_id_type=MESH,
        ).start()

    pending = []
    for s in range(len(ORDER)):
        if s == LAST:
            mine.wait()
        n = tms - 1 if s == LAST else tms
        landed = raw.at[pl.ds(s * tms, n)]
        pltpu.make_async_remote_copy(
            src_ref=landed, dst_ref=landed, send_sem=send1, recv_sem=recv1.at[s],
            device_id=(t, m), device_id_type=MESH,
        ).wait_recv()
        transform(s)
        step = 4
        for lo in range(0, s + 1, step):
            hi = min(lo + step, s + 1)

            @pl.loop(lo, hi)
            def _(s2, s=s):
                block(s, s2)

            for a, b in pending:
                ship(a, b)
            pending = []
            for s2 in range(lo, hi):
                pending.append((s, s2))
                if s2 != s:
                    pending.append((s2, s))
    for a, b in pending:
        ship(a, b)
    for b in range(len(ORDER)):
        got[m, group[b]] = blk[LAST, b]

    arrived = got.at[pl.ds(0, members - 1)]
    done = pltpu.make_async_remote_copy(
        src_ref=arrived, dst_ref=arrived, send_sem=send3, recv_sem=recv3,
        device_id=(t, m), device_id_type=MESH,
    )
    done.wait_recv()

    @pl.loop(0, rows)
    def _(i):
        for o in range(members):
            for n in range(members):
                out[i, n * rows:(n + 1) * rows, o * 128:(o + 1) * 128] = got[o, n, i]

    done.wait_send()
    sent = raw.at[pl.ds(0, total - 1)]
    pltpu.make_async_remote_copy(
        src_ref=sent, dst_ref=sent, send_sem=send1, recv_sem=recv1.at[0],
        device_id=(t, m), device_id_type=MESH,
    ).wait_send()


def per_device(fields):
    rows, mons, pixels = fields.shape
    tms, members = lax.axis_size("tm"), lax.axis_size("member")
    scale = 1.0 / (8.0 * float(mons * tms - 12))
    return pl.pallas_call(
        functools.partial(kernel, (tms, members, rows, mons, scale)),
        out_shape=jax.ShapeDtypeStruct((rows, rows * members, pixels // tms), F32),
        in_specs=[pl.BlockSpec(memory_space=pltpu.HBM)],
        out_specs=pl.BlockSpec(memory_space=pltpu.VMEM),
        scratch_shapes=[
            pltpu.VMEM((tms * members, rows, mons, 128), F32),
            pltpu.VMEM((members, 14, rows, 8, 128), F32),
            pltpu.VMEM((members, members, rows, rows, 128), F32),
            pltpu.VMEM((members, members, rows, rows, 128), F32),
            pltpu.SemaphoreType.DMA,
            pltpu.SemaphoreType.DMA((members,)),
            pltpu.SemaphoreType.DMA,
            pltpu.SemaphoreType.DMA,
            pltpu.SemaphoreType.DMA,
        ],
        compiler_params=pltpu.CompilerParams(collective_id=0, has_side_effects=True, vmem_limit_bytes=40 * 2**20),
        name="cov",
    )(fields)


def solution(mesh):
    in_specs = (P("member", "tm", None),)
    out_specs = P("member", None, "tm")
    return jax.shard_map(per_device, mesh=mesh, in_specs=in_specs, out_specs=out_specs, check_vma=False)
```

```python
import functools

import jax
import jax.numpy as jnp
from jax import lax
from jax.experimental import pallas as pl
from jax.experimental.pallas import tpu as pltpu
from jax.sharding import PartitionSpec as P

MESH = pl.DeviceIdType.MESH
F32 = jnp.float32
ORDER = ((1, 1), (3, 0), (1, 0), (3, 1), (0, 0), (2, 1), (0, 1), (2, 0))
SELF = ORDER.index((0, 0))
SENDS = (
    (1, 1), (0, 9), (1, 0), (0, 8), (0, 3), (1, 10), (1, 13), (0, 5), (1, 4), (0, 12), (1, 3), (0, 10),
    (1, 5), (0, 13), (1, 11), (0, 2), (0, 4), (1, 12), (1, 2), (0, 11), (0, 7), (1, 14), (0, 0), (1, 9),
    (0, 14), (1, 7), (1, 6), (0, 15), (0, 6), (1, 15), (0, 1), (1, 8), (2, 0), (3, 9), (2, 1), (3, 8),
    (2, 3), (3, 10), (3, 13), (2, 5), (3, 4), (2, 12), (3, 3), (2, 10), (3, 5), (2, 13), (3, 11), (2, 2),
    (2, 4), (3, 12), (3, 2), (2, 11), (2, 7), (3, 14), (2, 14), (3, 7), (3, 1), (2, 9), (3, 6), (2, 15),
    (2, 6), (3, 15), (3, 0), (2, 8), (5, 9), (4, 1), (5, 8), (4, 4), (5, 13), (4, 2), (5, 10), (4, 5),
    (5, 12), (4, 13), (5, 5), (4, 3), (5, 11), (4, 12), (5, 4), (4, 15), (5, 7), (4, 6), (5, 14), (4, 7),
    (5, 15), (4, 8), (5, 0), (4, 14), (5, 6), (4, 9), (5, 1), (5, 3), (4, 10), (4, 11), (5, 2), (6, 3),
    (7, 10), (6, 2), (7, 11), (7, 7), (6, 14), (7, 0), (6, 9), (7, 14), (6, 7), (6, 1), (7, 9), (6, 6),
    (7, 15), (7, 6), (6, 15), (6, 0), (7, 8), (7, 1), (6, 8), (7, 3), (6, 10), (6, 13), (7, 5), (6, 4),
    (7, 12), (6, 5), (7, 13), (6, 11), (7, 2), (7, 4), (6, 12),
)


def contrasts(years):
    shifted = [y - years[0] for y in years[1:]]
    a1, a2, a3, a4, a5, a6, a7 = shifted
    p0, m0 = a4, -a4
    p1, m1 = a1 + a5, a1 - a5
    p2, m2 = a2 + a6, a2 - a6
    p3, m3 = a3 + a7, a3 - a7
    out = []
    q0, q2, q1, q3 = p0 + p2, p0 - p2, p1 + p3, p1 - p3
    out += [q0 - q1, q2 + q3, q2 - q3]
    r0, r2, r1, r3 = m0 + m2, m0 - m2, m1 + m3, m1 - m3
    out += [r0 + r1, r0 - r1, r2 + r3, r2 - r3]
    return out


def kernel(sizes, fields, out, raw, con, blk, got, send1, recv1, own, send3, recv3):
    tms, members, rows, mons, scale = sizes
    t, m = lax.axis_index("tm"), lax.axis_index("member")
    me = t * members + m
    total = tms * members
    x, h = m // 2, m % 2
    ten, low, core = t // 4, (t // 2) % 2, t % 2

    barrier = pltpu.get_barrier_semaphore()

    near_t = [((ten + q // 4) % 4) * 4 + ((low + (q // 2) % 2) % 2) * 2 + (core + q % 2) % 2 for q in range(tms)]
    from_m = [((x + dx) % 4) * 2 + (h + dh) % 2 for dx, dh in ORDER]
    to_m = [((x + 4 - dx) % 4) * 2 + (h + dh) % 2 for dx, dh in ORDER]

    for s, q in SENDS:
        pl.semaphore_signal(barrier, inc=1, device_id=(near_t[q], to_m[s]), device_id_type=MESH)

    def pixels(d):
        return pl.ds(pl.multiple_of(d * 128, 128), 128)

    mine = pltpu.make_async_copy(fields.at[:, :, pixels(me)], raw.at[SELF * tms + t], own)
    mine.start()

    @pl.loop(0, con.shape[0])
    def _(s):
        con[s] = jnp.zeros(con.shape[1:], F32)

    pl.semaphore_wait(barrier, total - 1)

    for s, q in SENDS:
        pltpu.make_async_remote_copy(
            src_ref=fields.at[:, :, pixels(near_t[q] * members + to_m[s])],
            dst_ref=raw.at[s * tms + t],
            send_sem=send1,
            recv_sem=recv1.at[s],
            device_id=(near_t[q], to_m[s]),
            device_id_type=MESH,
        ).start()

    def transform(s):
        @pl.loop(0, rows)
        def _(i):
            for half in range(2):
                years = [raw[s * tms + 2 * y + half, i] for y in range(tms // 2)]
                for q, c in enumerate(contrasts(years)):
                    con[s, half * 7 + q, i, 0:mons] = c

    lane_row = lax.broadcasted_iota(jnp.int32, (8, 128), 0)

    def block(s, s2):
        cols = [jnp.zeros((8, 128), F32) for _ in range(rows)]
        for base in range(0, rows, 3):
            acc = [[None] * rows for _ in range(3)]
            for q in range(14):
                left = [con[s, q, base + a] for a in range(3)]
                right = [con[s2, q, b] for b in range(rows)]
                for a in range(3):
                    for b in range(rows):
                        prod = left[a] * right[b]
                        acc[a][b] = prod if q == 0 else acc[a][b] + prod
            for a in range(3):
                line = jnp.zeros((8, 128), F32)
                for b in range(rows):
                    r = jnp.sum(acc[a][b], axis=0, keepdims=True) * scale
                    r = jnp.broadcast_to(r, (8, 128))
                    line = jnp.where(lane_row == b, r, line)
                    cols[b] = jnp.where(lane_row == base + a, r, cols[b])
                blk[s, s2, base + a] = line[0:rows]
        for b in range(rows):
            blk[s2, s, b] = cols[b][0:rows]

    def ship(a, b):
        if a == SELF:
            return
        pltpu.make_async_remote_copy(
            src_ref=blk.at[a, b],
            dst_ref=got.at[m, from_m[b]],
            send_sem=send3,
            recv_sem=recv3,
            device_id=(t, from_m[a]),
            device_id_type=MESH,
        ).start()

    pending = []
    for s in range(len(ORDER)):
        if s == SELF:
            mine.wait()
        n = tms - 1 if s == SELF else tms
        landed = raw.at[pl.ds(s * tms, n)]
        pltpu.make_async_remote_copy(
            src_ref=landed, dst_ref=landed, send_sem=send1, recv_sem=recv1.at[s],
            device_id=(t, m), device_id_type=MESH,
        ).wait_recv()
        transform(s)
        step = 4
        for lo in range(0, s + 1, step):
            hi = min(lo + step, s + 1)

            @pl.loop(lo, hi)
            def _(s2, s=s):
                block(s, s2)

            for a, b in pending:
                ship(a, b)
            pending = []
            for s2 in range(lo, hi):
                pending.append((s, s2))
                if s2 != s:
                    pending.append((s2, s))
    for a, b in pending:
        ship(a, b)
    for b in range(len(ORDER)):
        got[m, from_m[b]] = blk[SELF, b]

    arrived = got.at[pl.ds(0, members - 1)]
    done = pltpu.make_async_remote_copy(
        src_ref=arrived, dst_ref=arrived, send_sem=send3, recv_sem=recv3,
        device_id=(t, m), device_id_type=MESH,
    )
    done.wait_recv()

    @pl.loop(0, rows)
    def _(i):
        for o in range(members):
            for n in range(members):
                out[i, n * rows:(n + 1) * rows, o * 128:(o + 1) * 128] = got[o, n, i]

    done.wait_send()
    sent = raw.at[pl.ds(0, total - 1)]
    pltpu.make_async_remote_copy(
        src_ref=sent, dst_ref=sent, send_sem=send1, recv_sem=recv1.at[0],
        device_id=(t, m), device_id_type=MESH,
    ).wait_send()


def per_device(fields):
    rows, mons, pixels = fields.shape
    tms, members = lax.axis_size("tm"), lax.axis_size("member")
    scale = 1.0 / (8.0 * float(mons * tms - 12))
    return pl.pallas_call(
        functools.partial(kernel, (tms, members, rows, mons, scale)),
        out_shape=jax.ShapeDtypeStruct((rows, rows * members, pixels // tms), F32),
        in_specs=[pl.BlockSpec(memory_space=pltpu.HBM)],
        out_specs=pl.BlockSpec(memory_space=pltpu.VMEM),
        scratch_shapes=[
            pltpu.VMEM((tms * members, rows, mons, 128), F32),
            pltpu.VMEM((members, 14, rows, 8, 128), F32),
            pltpu.VMEM((members, members, rows, rows, 128), F32),
            pltpu.VMEM((members, members, rows, rows, 128), F32),
            pltpu.SemaphoreType.DMA,
            pltpu.SemaphoreType.DMA((members,)),
            pltpu.SemaphoreType.DMA,
            pltpu.SemaphoreType.DMA,
            pltpu.SemaphoreType.DMA,
        ],
        compiler_params=pltpu.CompilerParams(collective_id=0, has_side_effects=True, vmem_limit_bytes=40 * 2**20),
        name="cov",
    )(fields)


def solution(mesh):
    in_specs = (P("member", "tm", None),)
    out_specs = P("member", None, "tm")
    return jax.shard_map(per_device, mesh=mesh, in_specs=in_specs, out_specs=out_specs, check_vma=False)
```

```python
import functools

import jax
import jax.numpy as jnp
from jax import lax
from jax.experimental import pallas as pl
from jax.experimental.pallas import tpu as pltpu
from jax.sharding import PartitionSpec as P

MESH = pl.DeviceIdType.MESH
F32 = jnp.float32
ORDER = ((2, 1), (0, 0), (2, 0), (0, 1), (1, 1), (3, 0), (1, 0), (3, 1))
SELF = ORDER.index((0, 0))
SENDS = (
    (0, 9), (1, 1), (0, 8), (1, 4), (0, 13), (1, 2), (0, 10), (1, 5), (0, 12), (1, 13), (0, 5), (1, 3),
    (0, 11), (1, 12), (0, 4), (1, 15), (0, 7), (1, 6), (0, 14), (1, 7), (0, 15), (1, 8), (0, 0), (1, 14),
    (0, 6), (1, 9), (0, 1), (0, 3), (1, 10), (1, 11), (0, 2), (3, 3), (2, 10), (3, 2), (2, 11), (2, 7),
    (3, 14), (2, 0), (3, 9), (2, 14), (3, 7), (3, 1), (2, 9), (3, 6), (2, 15), (2, 6), (3, 15), (3, 0),
    (2, 8), (2, 1), (3, 8), (2, 3), (3, 10), (3, 13), (2, 5), (3, 4), (2, 12), (3, 5), (2, 13), (3, 11),
    (2, 2), (2, 4), (3, 12), (5, 1), (4, 9), (5, 0), (4, 8), (4, 3), (5, 10), (5, 13), (4, 5), (5, 4),
    (4, 12), (5, 3), (4, 10), (5, 5), (4, 13), (5, 11), (4, 2), (4, 4), (5, 12), (5, 2), (4, 11), (4, 7),
    (5, 14), (4, 0), (5, 9), (4, 14), (5, 7), (5, 6), (4, 15), (4, 6), (5, 15), (4, 1), (5, 8), (6, 0),
    (7, 9), (6, 1), (7, 8), (6, 3), (7, 10), (7, 13), (6, 5), (7, 4), (6, 12), (7, 3), (6, 10), (7, 5),
    (6, 13), (7, 11), (6, 2), (6, 4), (7, 12), (7, 2), (6, 11), (6, 7), (7, 14), (6, 14), (7, 7), (7, 1),
    (6, 9), (7, 6), (6, 15), (6, 6), (7, 15), (7, 0), (6, 8),
)


def contrasts(years):
    shifted = [y - years[0] for y in years[1:]]
    a1, a2, a3, a4, a5, a6, a7 = shifted
    p0, m0 = a4, -a4
    p1, m1 = a1 + a5, a1 - a5
    p2, m2 = a2 + a6, a2 - a6
    p3, m3 = a3 + a7, a3 - a7
    out = []
    q0, q2, q1, q3 = p0 + p2, p0 - p2, p1 + p3, p1 - p3
    out += [q0 - q1, q2 + q3, q2 - q3]
    r0, r2, r1, r3 = m0 + m2, m0 - m2, m1 + m3, m1 - m3
    out += [r0 + r1, r0 - r1, r2 + r3, r2 - r3]
    return out


def kernel(sizes, fields, out, raw, con, blk, got, send1, recv1, own, send3, recv3):
    tms, members, rows, mons, scale = sizes
    t, m = lax.axis_index("tm"), lax.axis_index("member")
    me = t * members + m
    total = tms * members
    x, h = m // 2, m % 2
    ten, low, core = t // 4, (t // 2) % 2, t % 2

    barrier = pltpu.get_barrier_semaphore()

    near_t = [((ten + q // 4) % 4) * 4 + ((low + (q // 2) % 2) % 2) * 2 + (core + q % 2) % 2 for q in range(tms)]
    from_m = [((x + dx) % 4) * 2 + (h + dh) % 2 for dx, dh in ORDER]
    to_m = [((x + 4 - dx) % 4) * 2 + (h + dh) % 2 for dx, dh in ORDER]

    for s, q in SENDS:
        pl.semaphore_signal(barrier, inc=1, device_id=(near_t[q], to_m[s]), device_id_type=MESH)

    def pixels(d):
        return pl.ds(pl.multiple_of(d * 128, 128), 128)

    mine = pltpu.make_async_copy(fields.at[:, :, pixels(me)], raw.at[SELF * tms + t], own)
    mine.start()

    @pl.loop(0, con.shape[0])
    def _(s):
        con[s] = jnp.zeros(con.shape[1:], F32)

    pl.semaphore_wait(barrier, total - 1)

    for s, q in SENDS:
        pltpu.make_async_remote_copy(
            src_ref=fields.at[:, :, pixels(near_t[q] * members + to_m[s])],
            dst_ref=raw.at[s * tms + t],
            send_sem=send1,
            recv_sem=recv1.at[s],
            device_id=(near_t[q], to_m[s]),
            device_id_type=MESH,
        ).start()

    def transform(s):
        @pl.loop(0, rows)
        def _(i):
            for half in range(2):
                years = [raw[s * tms + 2 * y + half, i] for y in range(tms // 2)]
                for q, c in enumerate(contrasts(years)):
                    con[s, half * 7 + q, i, 0:mons] = c

    lane_row = lax.broadcasted_iota(jnp.int32, (8, 128), 0)

    def block(s, s2):
        cols = [jnp.zeros((8, 128), F32) for _ in range(rows)]
        for base in range(0, rows, 3):
            acc = [[None] * rows for _ in range(3)]
            for q in range(14):
                left = [con[s, q, base + a] for a in range(3)]
                right = [con[s2, q, b] for b in range(rows)]
                for a in range(3):
                    for b in range(rows):
                        prod = left[a] * right[b]
                        acc[a][b] = prod if q == 0 else acc[a][b] + prod
            for a in range(3):
                line = jnp.zeros((8, 128), F32)
                for b in range(rows):
                    r = jnp.sum(acc[a][b], axis=0, keepdims=True) * scale
                    r = jnp.broadcast_to(r, (8, 128))
                    line = jnp.where(lane_row == b, r, line)
                    cols[b] = jnp.where(lane_row == base + a, r, cols[b])
                blk[s, s2, base + a] = line[0:rows]
        for b in range(rows):
            blk[s2, s, b] = cols[b][0:rows]

    def ship(a, b):
        if a == SELF:
            return
        pltpu.make_async_remote_copy(
            src_ref=blk.at[a, b],
            dst_ref=got.at[m, from_m[b]],
            send_sem=send3,
            recv_sem=recv3.at[m],
            device_id=(t, from_m[a]),
            device_id_type=MESH,
        ).start()

    pending = []
    for s in range(len(ORDER)):
        if s == SELF:
            mine.wait()
        n = tms - 1 if s == SELF else tms
        landed = raw.at[pl.ds(s * tms, n)]
        pltpu.make_async_remote_copy(
            src_ref=landed, dst_ref=landed, send_sem=send1, recv_sem=recv1.at[s],
            device_id=(t, m), device_id_type=MESH,
        ).wait_recv()
        transform(s)
        step = 4
        for lo in range(0, s + 1, step):
            hi = min(lo + step, s + 1)

            @pl.loop(lo, hi)
            def _(s2, s=s):
                block(s, s2)

            for a, b in pending:
                ship(a, b)
            pending = []
            for s2 in range(lo, hi):
                pending.append((s, s2))
                if s2 != s:
                    pending.append((s2, s))
    for a, b in pending:
        ship(a, b)
    def place(o, line):
        lanes = pixels(o)

        @pl.loop(0, rows)
        def _(i):
            for n in range(members):
                out[i, n * rows:(n + 1) * rows, lanes] = line(n, i)

    for b in range(len(ORDER)):
        got[m, from_m[b]] = blk[SELF, b]
    for o in [m] + [from_m[b] for b in range(len(ORDER)) if b != SELF]:
        if o is not m:
            part = got.at[o]
            pltpu.make_async_remote_copy(
                src_ref=part, dst_ref=part, send_sem=send3, recv_sem=recv3.at[o],
                device_id=(t, m), device_id_type=MESH,
            ).wait_recv()
        place(o, lambda n, i, o=o: got[o, n, i])

    shipped = got.at[pl.ds(0, members - 1)]
    pltpu.make_async_remote_copy(
        src_ref=shipped, dst_ref=shipped, send_sem=send3, recv_sem=recv3.at[0],
        device_id=(t, m), device_id_type=MESH,
    ).wait_send()
    sent = raw.at[pl.ds(0, total - 1)]
    pltpu.make_async_remote_copy(
        src_ref=sent, dst_ref=sent, send_sem=send1, recv_sem=recv1.at[0],
        device_id=(t, m), device_id_type=MESH,
    ).wait_send()


def per_device(fields):
    rows, mons, pixels = fields.shape
    tms, members = lax.axis_size("tm"), lax.axis_size("member")
    scale = 1.0 / (8.0 * float(mons * tms - 12))
    return pl.pallas_call(
        functools.partial(kernel, (tms, members, rows, mons, scale)),
        out_shape=jax.ShapeDtypeStruct((rows, rows * members, pixels // tms), F32),
        in_specs=[pl.BlockSpec(memory_space=pltpu.HBM)],
        out_specs=pl.BlockSpec(memory_space=pltpu.VMEM),
        scratch_shapes=[
            pltpu.VMEM((tms * members, rows, mons, 128), F32),
            pltpu.VMEM((members, 14, rows, 8, 128), F32),
            pltpu.VMEM((members, members, rows, rows, 128), F32),
            pltpu.VMEM((members, members, rows, rows, 128), F32),
            pltpu.SemaphoreType.DMA,
            pltpu.SemaphoreType.DMA((members,)),
            pltpu.SemaphoreType.DMA,
            pltpu.SemaphoreType.DMA,
            pltpu.SemaphoreType.DMA((members,)),
        ],
        compiler_params=pltpu.CompilerParams(collective_id=0, has_side_effects=True, vmem_limit_bytes=50 * 2**20),
        name="cov",
    )(fields)


def solution(mesh):
    in_specs = (P("member", "tm", None),)
    out_specs = P("member", None, "tm")
    return jax.shard_map(per_device, mesh=mesh, in_specs=in_specs, out_specs=out_specs, check_vma=False)
```

```python
import functools

import jax
import jax.numpy as jnp
from jax import lax
from jax.experimental import pallas as pl
from jax.experimental.pallas import tpu as pltpu
from jax.sharding import PartitionSpec as P

MESH = pl.DeviceIdType.MESH
F32 = jnp.float32
ORDER = ((2, 1), (0, 0), (2, 0), (0, 1), (1, 1), (3, 0), (1, 0), (3, 1))
EARLY = 7
SELF = ORDER.index((0, 0))
SENDS = (
    (0, 1), (1, 1), (0, 0), (2, 1), (3, 0), (2, 0), (3, 1), (1, 11), (0, 3), (1, 10), (0, 2), (0, 9),
    (1, 5), (0, 15), (1, 6), (0, 14), (1, 14), (0, 5), (1, 8), (1, 3), (0, 11), (0, 8), (1, 13), (0, 4),
    (1, 12), (1, 4), (0, 12), (0, 7), (1, 15), (0, 6), (1, 7), (0, 13), (1, 9), (1, 2), (0, 10), (3, 11),
    (2, 3), (3, 10), (2, 2), (2, 9), (3, 5), (2, 15), (3, 6), (2, 14), (3, 14), (2, 5), (3, 8), (3, 3),
    (2, 11), (2, 8), (3, 13), (2, 4), (3, 12), (3, 4), (2, 12), (2, 7), (3, 15), (2, 6), (3, 7), (2, 13),
    (3, 9), (3, 2), (2, 10), (4, 3), (5, 10), (4, 7), (5, 14), (5, 13), (4, 5), (5, 4), (4, 12), (5, 3),
    (4, 10), (4, 0), (5, 9), (4, 14), (5, 7), (5, 1), (4, 9), (5, 5), (4, 13), (5, 11), (4, 2), (5, 6),
    (4, 15), (4, 4), (5, 12), (4, 6), (5, 15), (5, 2), (4, 11), (5, 0), (4, 8), (4, 1), (5, 8), (6, 3),
    (7, 10), (6, 7), (7, 14), (7, 13), (6, 5), (7, 4), (6, 12), (7, 3), (6, 10), (6, 0), (7, 9), (6, 14),
    (7, 7), (7, 1), (6, 9), (7, 5), (6, 13), (7, 11), (6, 2), (7, 6), (6, 15), (6, 4), (7, 12), (6, 6),
    (7, 15), (7, 2), (6, 11), (7, 0), (6, 8), (6, 1), (7, 8),
)


def contrasts(years):
    shifted = [y - years[0] for y in years[1:]]
    a1, a2, a3, a4, a5, a6, a7 = shifted
    p0, m0 = a4, -a4
    p1, m1 = a1 + a5, a1 - a5
    p2, m2 = a2 + a6, a2 - a6
    p3, m3 = a3 + a7, a3 - a7
    out = []
    q0, q2, q1, q3 = p0 + p2, p0 - p2, p1 + p3, p1 - p3
    out += [q0 - q1, q2 + q3, q2 - q3]
    r0, r2, r1, r3 = m0 + m2, m0 - m2, m1 + m3, m1 - m3
    out += [r0 + r1, r0 - r1, r2 + r3, r2 - r3]
    return out


def kernel(sizes, fields, out, raw, con, blk, got, send1, recv1, own, send3, recv3, ready):
    tms, members, rows, mons, scale = sizes
    t, m = lax.axis_index("tm"), lax.axis_index("member")
    me = t * members + m
    total = tms * members
    x, h = m // 2, m % 2
    ten, low, core = t // 4, (t // 2) % 2, t % 2

    barrier = pltpu.get_barrier_semaphore()

    near_t = [((ten + q // 4) % 4) * 4 + ((low + (q // 2) % 2) % 2) * 2 + (core + q % 2) % 2 for q in range(tms)]
    from_m = [((x + dx) % 4) * 2 + (h + dh) % 2 for dx, dh in ORDER]
    to_m = [((x + 4 - dx) % 4) * 2 + (h + dh) % 2 for dx, dh in ORDER]

    def greet(other_t, other_m):
        pl.semaphore_signal(barrier, inc=1, device_id=(other_t, other_m), device_id_type=MESH)

    twin = t + 1 - 2 * core
    for s in range(len(ORDER)):
        for q in range(0, 4, 2):
            seen = near_t[q] - core
            if s == SELF and q == 0:
                pl.when(core == 1)(functools.partial(greet, seen, m))
            else:
                greet(seen, to_m[s])
    for s in range(len(ORDER)):
        for q in range(0, tms, 2):
            seen = near_t[q] + 1 - core
            if s == SELF and q == 0:
                pl.when(core == 0)(functools.partial(greet, seen, m))
            else:
                greet(seen, to_m[s])

    def pixels(d):
        return pl.ds(pl.multiple_of(d * 128, 128), 128)

    mine = pltpu.make_async_copy(fields.at[:, :, pixels(me)], raw.at[SELF * tms + t], own)
    mine.start()

    def send(s, q):
        pltpu.make_async_remote_copy(
            src_ref=fields.at[:, :, pixels(near_t[q] * members + to_m[s])],
            dst_ref=raw.at[s * tms + t],
            send_sem=send1,
            recv_sem=recv1.at[s],
            device_id=(near_t[q], to_m[s]),
            device_id_type=MESH,
        ).start()

    @pl.when(core == 0)
    def _():
        pl.semaphore_wait(barrier, 4 * members - 1)
        pl.semaphore_signal(ready, inc=1, device_id=(twin, m), device_id_type=MESH)

    @pl.when(core == 1)
    def _():
        pl.semaphore_wait(ready, 1)

    for s, q in SENDS[:EARLY]:
        send(s, q)

    @pl.when(core == 1)
    def _():
        pl.semaphore_wait(barrier, total - 1)
        pl.semaphore_signal(ready, inc=1, device_id=(twin, m), device_id_type=MESH)

    @pl.when(core == 0)
    def _():
        pl.semaphore_wait(ready, 1)

    for s, q in SENDS[EARLY:]:
        send(s, q)

    @pl.loop(0, con.shape[0])
    def _(s):
        con[s] = jnp.zeros(con.shape[1:], F32)

    def transform(s):
        @pl.loop(0, rows)
        def _(i):
            for half in range(2):
                years = [raw[s * tms + 2 * y + half, i] for y in range(tms // 2)]
                for q, c in enumerate(contrasts(years)):
                    con[s, half * 7 + q, i, 0:mons] = c

    lane_row = lax.broadcasted_iota(jnp.int32, (8, 128), 0)

    def block(s, s2):
        cols = [jnp.zeros((8, 128), F32) for _ in range(rows)]
        for base in range(0, rows, 3):
            acc = [[None] * rows for _ in range(3)]
            for q in range(14):
                left = [con[s, q, base + a] for a in range(3)]
                right = [con[s2, q, b] for b in range(rows)]
                for a in range(3):
                    for b in range(rows):
                        prod = left[a] * right[b]
                        acc[a][b] = prod if q == 0 else acc[a][b] + prod
            for a in range(3):
                line = jnp.zeros((8, 128), F32)
                for b in range(rows):
                    r = jnp.sum(acc[a][b], axis=0, keepdims=True) * scale
                    r = jnp.broadcast_to(r, (8, 128))
                    line = jnp.where(lane_row == b, r, line)
                    cols[b] = jnp.where(lane_row == base + a, r, cols[b])
                blk[s, s2, base + a] = line[0:rows]
        for b in range(rows):
            blk[s2, s, b] = cols[b][0:rows]

    def ship(a, b):
        if a == SELF:
            return
        pltpu.make_async_remote_copy(
            src_ref=blk.at[a, b],
            dst_ref=got.at[m, from_m[b]],
            send_sem=send3,
            recv_sem=recv3.at[m],
            device_id=(t, from_m[a]),
            device_id_type=MESH,
        ).start()

    pending = []
    for s in range(len(ORDER)):
        if s == SELF:
            mine.wait()
        n = tms - 1 if s == SELF else tms
        landed = raw.at[pl.ds(s * tms, n)]
        pltpu.make_async_remote_copy(
            src_ref=landed, dst_ref=landed, send_sem=send1, recv_sem=recv1.at[s],
            device_id=(t, m), device_id_type=MESH,
        ).wait_recv()
        transform(s)
        step = 4
        for lo in range(0, s + 1, step):
            hi = min(lo + step, s + 1)

            @pl.loop(lo, hi)
            def _(s2, s=s):
                block(s, s2)

            for a, b in pending:
                ship(a, b)
            pending = []
            for s2 in range(lo, hi):
                pending.append((s, s2))
                if s2 != s:
                    pending.append((s2, s))
    for a, b in pending:
        ship(a, b)
    def place(o, line):
        lanes = pixels(o)

        @pl.loop(0, rows)
        def _(i):
            for n in range(members):
                out[i, n * rows:(n + 1) * rows, lanes] = line(n, i)

    for b in range(len(ORDER)):
        got[m, from_m[b]] = blk[SELF, b]
    for o in [m] + [from_m[b] for b in range(len(ORDER)) if b != SELF]:
        if o is not m:
            part = got.at[o]
            pltpu.make_async_remote_copy(
                src_ref=part, dst_ref=part, send_sem=send3, recv_sem=recv3.at[o],
                device_id=(t, m), device_id_type=MESH,
            ).wait_recv()
        place(o, lambda n, i, o=o: got[o, n, i])

    shipped = got.at[pl.ds(0, members - 1)]
    pltpu.make_async_remote_copy(
        src_ref=shipped, dst_ref=shipped, send_sem=send3, recv_sem=recv3.at[0],
        device_id=(t, m), device_id_type=MESH,
    ).wait_send()
    sent = raw.at[pl.ds(0, total - 1)]
    pltpu.make_async_remote_copy(
        src_ref=sent, dst_ref=sent, send_sem=send1, recv_sem=recv1.at[0],
        device_id=(t, m), device_id_type=MESH,
    ).wait_send()


def per_device(fields):
    rows, mons, pixels = fields.shape
    tms, members = lax.axis_size("tm"), lax.axis_size("member")
    scale = 1.0 / (8.0 * float(mons * tms - 12))
    return pl.pallas_call(
        functools.partial(kernel, (tms, members, rows, mons, scale)),
        out_shape=jax.ShapeDtypeStruct((rows, rows * members, pixels // tms), F32),
        in_specs=[pl.BlockSpec(memory_space=pltpu.HBM)],
        out_specs=pl.BlockSpec(memory_space=pltpu.VMEM),
        scratch_shapes=[
            pltpu.VMEM((tms * members, rows, mons, 128), F32),
            pltpu.VMEM((members, 14, rows, 8, 128), F32),
            pltpu.VMEM((members, members, rows, rows, 128), F32),
            pltpu.VMEM((members, members, rows, rows, 128), F32),
            pltpu.SemaphoreType.DMA,
            pltpu.SemaphoreType.DMA((members,)),
            pltpu.SemaphoreType.DMA,
            pltpu.SemaphoreType.DMA,
            pltpu.SemaphoreType.DMA((members,)),
            pltpu.SemaphoreType.REGULAR,
        ],
        compiler_params=pltpu.CompilerParams(collective_id=0, has_side_effects=True, vmem_limit_bytes=50 * 2**20),
        name="cov",
    )(fields)


def solution(mesh):
    in_specs = (P("member", "tm", None),)
    out_specs = P("member", None, "tm")
    return jax.shard_map(per_device, mesh=mesh, in_specs=in_specs, out_specs=out_specs, check_vma=False)
```

```python
import functools

import jax
import jax.numpy as jnp
from jax import lax
from jax.experimental import pallas as pl
from jax.experimental.pallas import tpu as pltpu
from jax.sharding import PartitionSpec as P

MESH = pl.DeviceIdType.MESH
F32 = jnp.float32
ORDER = ((2, 1), (0, 0), (2, 0), (0, 1), (1, 1), (3, 0), (1, 0), (3, 1))
EARLY = 8
SELF = ORDER.index((0, 0))
SENDS = (
    (4, 3), (5, 3), (1, 3), (0, 3), (2, 3), (3, 3), (7, 3), (6, 3), (0, 8), (1, 1), (0, 9), (1, 4),
    (0, 12), (1, 12), (0, 4), (1, 13), (0, 5), (1, 9), (0, 0), (1, 8), (0, 1), (1, 5), (0, 13), (1, 10),
    (0, 2), (1, 11), (0, 6), (1, 15), (0, 11), (1, 2), (0, 10), (1, 6), (0, 15), (1, 7), (0, 14), (1, 14),
    (0, 7), (3, 9), (2, 0), (3, 11), (2, 2), (2, 8), (3, 1), (2, 11), (3, 2), (2, 9), (3, 0), (3, 10),
    (2, 7), (3, 15), (2, 6), (3, 13), (2, 13), (3, 4), (2, 4), (3, 14), (2, 10), (2, 1), (3, 8), (3, 6),
    (2, 14), (3, 5), (2, 12), (3, 12), (2, 5), (3, 7), (2, 15), (5, 9), (4, 0), (5, 11), (4, 2), (4, 8),
    (5, 1), (4, 11), (5, 2), (4, 9), (5, 0), (5, 10), (4, 7), (5, 15), (4, 6), (5, 13), (4, 13), (5, 4),
    (4, 4), (5, 14), (4, 10), (4, 1), (5, 8), (5, 6), (4, 14), (5, 5), (4, 12), (5, 12), (4, 5), (5, 7),
    (4, 15), (7, 9), (6, 0), (7, 11), (6, 2), (6, 8), (7, 1), (6, 11), (7, 2), (6, 9), (7, 0), (7, 10),
    (6, 7), (7, 15), (6, 6), (7, 13), (6, 13), (7, 4), (6, 4), (7, 14), (6, 10), (6, 1), (7, 8), (7, 6),
    (6, 14), (7, 5), (6, 12), (7, 12), (6, 5), (7, 7), (6, 15),
)


def contrasts(years):
    shifted = [y - years[0] for y in years[1:]]
    a1, a2, a3, a4, a5, a6, a7 = shifted
    p0, m0 = a4, -a4
    p1, m1 = a1 + a5, a1 - a5
    p2, m2 = a2 + a6, a2 - a6
    p3, m3 = a3 + a7, a3 - a7
    out = []
    q0, q2, q1, q3 = p0 + p2, p0 - p2, p1 + p3, p1 - p3
    out += [q0 - q1, q2 + q3, q2 - q3]
    r0, r2, r1, r3 = m0 + m2, m0 - m2, m1 + m3, m1 - m3
    out += [r0 + r1, r0 - r1, r2 + r3, r2 - r3]
    return out


def kernel(sizes, fields, out, raw, con, blk, got, send1, recv1, own, send3, recv3, ready):
    tms, members, rows, mons, scale = sizes
    t, m = lax.axis_index("tm"), lax.axis_index("member")
    me = t * members + m
    total = tms * members
    x, h = m // 2, m % 2
    ten, low, core = t // 4, (t // 2) % 2, t % 2

    barrier = pltpu.get_barrier_semaphore()

    near_t = [((ten + q // 4) % 4) * 4 + ((low + (q // 2) % 2) % 2) * 2 + (core + q % 2) % 2 for q in range(tms)]
    from_m = [((x + dx) % 4) * 2 + (h + dh) % 2 for dx, dh in ORDER]
    to_m = [((x + 4 - dx) % 4) * 2 + (h + dh) % 2 for dx, dh in ORDER]

    def greet(other_t, other_m):
        pl.semaphore_signal(barrier, inc=1, device_id=(other_t, other_m), device_id_type=MESH)

    twin = t + 1 - 2 * core
    for s in range(len(ORDER)):
        for q in range(0, 4, 2):
            seen = near_t[q] - core
            if s == SELF and q == 0:
                pl.when(core == 1)(functools.partial(greet, seen, m))
            else:
                greet(seen, to_m[s])
    for s in range(len(ORDER)):
        for q in range(0, tms, 2):
            seen = near_t[q] + 1 - core
            if s == SELF and q == 0:
                pl.when(core == 0)(functools.partial(greet, seen, m))
            else:
                greet(seen, to_m[s])

    def pixels(d):
        return pl.ds(pl.multiple_of(d * 128, 128), 128)

    mine = pltpu.make_async_copy(fields.at[:, :, pixels(me)], raw.at[SELF * tms + t], own)
    mine.start()

    def send(s, q):
        pltpu.make_async_remote_copy(
            src_ref=fields.at[:, :, pixels(near_t[q] * members + to_m[s])],
            dst_ref=raw.at[s * tms + t],
            send_sem=send1,
            recv_sem=recv1.at[s],
            device_id=(near_t[q], to_m[s]),
            device_id_type=MESH,
        ).start()

    @pl.when(core == 0)
    def _():
        pl.semaphore_wait(barrier, 4 * members - 1)
        pl.semaphore_signal(ready, inc=1, device_id=(twin, m), device_id_type=MESH)

    @pl.when(core == 1)
    def _():
        pl.semaphore_wait(ready, 1)

    for s, q in SENDS[:EARLY]:
        send(s, q)

    @pl.when(core == 1)
    def _():
        pl.semaphore_wait(barrier, total - 1)
        pl.semaphore_signal(ready, inc=1, device_id=(twin, m), device_id_type=MESH)

    @pl.when(core == 0)
    def _():
        pl.semaphore_wait(ready, 1)

    for s, q in SENDS[EARLY:]:
        send(s, q)

    @pl.loop(0, con.shape[0])
    def _(s):
        con[s] = jnp.zeros(con.shape[1:], F32)

    def transform(s):
        @pl.loop(0, rows)
        def _(i):
            for half in range(2):
                years = [raw[s * tms + 2 * y + half, i] for y in range(tms // 2)]
                for q, c in enumerate(contrasts(years)):
                    con[s, half * 7 + q, i, 0:mons] = c

    lane_row = lax.broadcasted_iota(jnp.int32, (8, 128), 0)

    def block(s, s2):
        cols = [jnp.zeros((8, 128), F32) for _ in range(rows)]
        for base in range(0, rows, 3):
            acc = [[None] * rows for _ in range(3)]
            for q in range(14):
                left = [con[s, q, base + a] for a in range(3)]
                right = [con[s2, q, b] for b in range(rows)]
                for a in range(3):
                    for b in range(rows):
                        prod = left[a] * right[b]
                        acc[a][b] = prod if q == 0 else acc[a][b] + prod
            for a in range(3):
                line = jnp.zeros((8, 128), F32)
                for b in range(rows):
                    r = jnp.sum(acc[a][b], axis=0, keepdims=True) * scale
                    r = jnp.broadcast_to(r, (8, 128))
                    line = jnp.where(lane_row == b, r, line)
                    cols[b] = jnp.where(lane_row == base + a, r, cols[b])
                blk[s, s2, base + a] = line[0:rows]
        for b in range(rows):
            blk[s2, s, b] = cols[b][0:rows]

    def pack(s):
        r3, r4, r5 = (blk[s, s, i] for i in range(3, 6))
        blk[s, s, 3] = jnp.concatenate([r3[3:6], r4[4:6], r5[5:6]], axis=0)

    def unpack(o):
        top = [got[o, m * rows + i] for i in range(3)]
        low = got[o, m * rows + 3]
        for i, rest in ((3, [low[0:3]]), (4, [low[1:2], low[3:5]]), (5, [low[2:3], low[4:6]])):
            got[o, m * rows + i] = jnp.concatenate([r[i:i + 1] for r in top] + rest, axis=0)

    def ship(a, b):
        if a == SELF:
            return
        lines = 4 if a == b else rows
        pltpu.make_async_remote_copy(
            src_ref=blk.at[a, b, pl.ds(0, lines)],
            dst_ref=got.at[m, pl.ds(from_m[b] * rows, lines)],
            send_sem=send3,
            recv_sem=recv3.at[m],
            device_id=(t, from_m[a]),
            device_id_type=MESH,
        ).start()

    pending = []
    for s in range(len(ORDER)):
        if s == SELF:
            mine.wait()
        n = tms - 1 if s == SELF else tms
        landed = raw.at[pl.ds(s * tms, n)]
        pltpu.make_async_remote_copy(
            src_ref=landed, dst_ref=landed, send_sem=send1, recv_sem=recv1.at[s],
            device_id=(t, m), device_id_type=MESH,
        ).wait_recv()
        transform(s)
        step = 4
        for lo in range(0, s + 1, step):
            hi = min(lo + step, s + 1)

            @pl.loop(lo, hi)
            def _(s2, s=s):
                block(s, s2)

            if hi == s + 1 and s != SELF:
                pack(s)
            for a, b in pending:
                ship(a, b)
            pending = []
            for s2 in range(lo, hi):
                pending.append((s, s2))
                if s2 != s:
                    pending.append((s2, s))
    for a, b in pending:
        ship(a, b)
    def place(o, line):
        lanes = pixels(o)

        @pl.loop(0, rows)
        def _(i):
            for n in range(members):
                out[i, n * rows:(n + 1) * rows, lanes] = line(n, i)

    for b in range(len(ORDER)):
        got[m, pl.ds(from_m[b] * rows, rows)] = blk[SELF, b]
    for o in [m] + [from_m[b] for b in range(len(ORDER)) if b != SELF]:
        if o is not m:
            part = got.at[o, pl.ds(0, members * rows - 2)]
            pltpu.make_async_remote_copy(
                src_ref=part, dst_ref=part, send_sem=send3, recv_sem=recv3.at[o],
                device_id=(t, m), device_id_type=MESH,
            ).wait_recv()
            unpack(o)
        place(o, lambda n, i, o=o: got[o, n * rows + i])

    shipped = got.at[pl.ds(0, members - 1), pl.ds(0, members * rows - 2)]
    pltpu.make_async_remote_copy(
        src_ref=shipped, dst_ref=shipped, send_sem=send3, recv_sem=recv3.at[0],
        device_id=(t, m), device_id_type=MESH,
    ).wait_send()
    sent = raw.at[pl.ds(0, total - 1)]
    pltpu.make_async_remote_copy(
        src_ref=sent, dst_ref=sent, send_sem=send1, recv_sem=recv1.at[0],
        device_id=(t, m), device_id_type=MESH,
    ).wait_send()


def per_device(fields):
    rows, mons, pixels = fields.shape
    tms, members = lax.axis_size("tm"), lax.axis_size("member")
    scale = 1.0 / (8.0 * float(mons * tms - 12))
    return pl.pallas_call(
        functools.partial(kernel, (tms, members, rows, mons, scale)),
        out_shape=jax.ShapeDtypeStruct((rows, rows * members, pixels // tms), F32),
        in_specs=[pl.BlockSpec(memory_space=pltpu.HBM)],
        out_specs=pl.BlockSpec(memory_space=pltpu.VMEM),
        scratch_shapes=[
            pltpu.VMEM((tms * members, rows, mons, 128), F32),
            pltpu.VMEM((members, 14, rows, 8, 128), F32),
            pltpu.VMEM((members, members, rows, rows, 128), F32),
            pltpu.VMEM((members, members * rows, rows, 128), F32),
            pltpu.SemaphoreType.DMA,
            pltpu.SemaphoreType.DMA((members,)),
            pltpu.SemaphoreType.DMA,
            pltpu.SemaphoreType.DMA,
            pltpu.SemaphoreType.DMA((members,)),
            pltpu.SemaphoreType.REGULAR,
        ],
        compiler_params=pltpu.CompilerParams(collective_id=0, has_side_effects=True, vmem_limit_bytes=50 * 2**20),
        name="cov",
    )(fields)


def solution(mesh):
    in_specs = (P("member", "tm", None),)
    out_specs = P("member", None, "tm")
    return jax.shard_map(per_device, mesh=mesh, in_specs=in_specs, out_specs=out_specs, check_vma=False)
```

```python
import functools

import jax
import jax.numpy as jnp
from jax import lax
from jax.experimental import pallas as pl
from jax.experimental.pallas import tpu as pltpu
from jax.sharding import PartitionSpec as P

MESH = pl.DeviceIdType.MESH
F32 = jnp.float32
ORDER = ((2, 1), (0, 0), (2, 0), (0, 1), (1, 1), (3, 0), (1, 0), (3, 1))
SELF = ORDER.index((0, 0))
SENDS = (
    (4, 3), (5, 3), (1, 3), (0, 3), (2, 3), (3, 3), (7, 3), (6, 3), (0, 8), (1, 1), (0, 9), (1, 12),
    (0, 4), (1, 4), (0, 12), (1, 13), (0, 5), (1, 8), (0, 1), (1, 9), (0, 0), (1, 5), (0, 13), (1, 10),
    (0, 2), (1, 11), (0, 6), (1, 15), (0, 10), (1, 2), (0, 11), (1, 6), (0, 14), (1, 7), (0, 15), (1, 14),
    (0, 7), (3, 9), (2, 0), (3, 11), (2, 2), (2, 8), (3, 1), (2, 11), (3, 2), (2, 9), (3, 0), (3, 10),
    (2, 7), (3, 15), (2, 6), (3, 13), (2, 13), (3, 4), (2, 4), (3, 14), (2, 10), (2, 1), (3, 8), (3, 6),
    (2, 14), (3, 5), (2, 12), (3, 12), (2, 5), (3, 7), (2, 15), (5, 9), (4, 0), (5, 11), (4, 2), (4, 8),
    (5, 1), (4, 11), (5, 2), (4, 9), (5, 0), (5, 10), (4, 7), (5, 15), (4, 6), (5, 13), (4, 13), (5, 4),
    (4, 4), (5, 14), (4, 10), (4, 1), (5, 8), (5, 6), (4, 14), (5, 5), (4, 12), (5, 12), (4, 5), (5, 7),
    (4, 15), (7, 9), (6, 0), (7, 11), (6, 2), (6, 8), (7, 1), (6, 11), (7, 2), (6, 9), (7, 0), (7, 10),
    (6, 7), (7, 15), (6, 6), (7, 13), (6, 13), (7, 4), (6, 4), (7, 14), (6, 10), (6, 1), (7, 8), (7, 6),
    (6, 14), (7, 5), (6, 12), (7, 12), (6, 5), (7, 7), (6, 15),
)
FIRST = (
    4, 4, 4, 4, 4, 4, 4, 4, 0, 0, 0, 0, 0, 0, 0, 0, 0, 0, 0, 0, 1, 0, 0, 0, 0, 0, 0, 0, 0, 0,
    0, 0, 0, 0, 0, 0, 0, 0, 1, 0, 0, 0, 0, 0, 0, 0, 2, 0, 0, 0, 0, 0, 0, 0, 0, 0, 0, 0, 0, 0,
    0, 0, 0, 0, 0, 0, 0, 0, 0, 0, 0, 0, 0, 0, 0, 0, 0, 0, 0, 0, 0, 0, 0, 0, 0, 0, 0, 0, 0, 0,
    0, 0, 0, 0, 0, 0, 0, 0, 0, 0, 0, 0, 0, 0, 0, 0, 0, 0, 0, 0, 0, 0, 0, 0, 0, 0, 0, 0, 0, 0,
    0, 0, 0, 0, 0, 0, 0,
)


def contrasts(years):
    shifted = [y - years[0] for y in years[1:]]
    a1, a2, a3, a4, a5, a6, a7 = shifted
    p0, m0 = a4, -a4
    p1, m1 = a1 + a5, a1 - a5
    p2, m2 = a2 + a6, a2 - a6
    p3, m3 = a3 + a7, a3 - a7
    out = []
    q0, q2, q1, q3 = p0 + p2, p0 - p2, p1 + p3, p1 - p3
    out += [q0 - q1, q2 + q3, q2 - q3]
    r0, r2, r1, r3 = m0 + m2, m0 - m2, m1 + m3, m1 - m3
    out += [r0 + r1, r0 - r1, r2 + r3, r2 - r3]
    return out


def kernel(sizes, fields, out, raw, con, blk, got, send1, recv1, own, send3, recv3, ready):
    tms, members, rows, mons, scale = sizes
    t, m = lax.axis_index("tm"), lax.axis_index("member")
    me = t * members + m
    total = tms * members
    x, h = m // 2, m % 2
    ten, low, core = t // 4, (t // 2) % 2, t % 2

    barrier = pltpu.get_barrier_semaphore()

    near_t = [((ten + q // 4) % 4) * 4 + ((low + (q // 2) % 2) % 2) * 2 + (core + q % 2) % 2 for q in range(tms)]
    from_m = [((x + dx) % 4) * 2 + (h + dh) % 2 for dx, dh in ORDER]
    to_m = [((x + 4 - dx) % 4) * 2 + (h + dh) % 2 for dx, dh in ORDER]

    def greet(other_t, other_m):
        pl.semaphore_signal(barrier, inc=1, device_id=(other_t, other_m), device_id_type=MESH)

    twin = t + 1 - 2 * core
    for s in range(len(ORDER)):
        for q in range(0, 4, 2):
            seen = near_t[q] - core
            if s == SELF and q == 0:
                pl.when(core == 1)(functools.partial(greet, seen, m))
            else:
                greet(seen, to_m[s])
    for s in range(len(ORDER)):
        for q in range(0, tms, 2):
            seen = near_t[q] + 1 - core
            if s == SELF and q == 0:
                pl.when(core == 0)(functools.partial(greet, seen, m))
            else:
                greet(seen, to_m[s])

    def pixels(d):
        return pl.ds(pl.multiple_of(d * 128, 128), 128)

    mine = pltpu.make_async_copy(fields.at[:, :, pixels(me)], raw.at[SELF * tms + t], own)
    mine.start()

    def send(s, q):
        pltpu.make_async_remote_copy(
            src_ref=fields.at[:, :, pixels(near_t[q] * members + to_m[s])],
            dst_ref=raw.at[s * tms + t],
            send_sem=send1,
            recv_sem=recv1.at[s],
            device_id=(near_t[q], to_m[s]),
            device_id_type=MESH,
        ).start()

    @pl.when(core == 0)
    def _():
        pl.semaphore_wait(barrier, 4 * members - 1)
        pl.semaphore_signal(ready, inc=1, device_id=(twin, m), device_id_type=MESH)

    @pl.when(core == 1)
    def _():
        pl.semaphore_wait(ready, 1)

    for (s, q), first in zip(SENDS, FIRST):
        if first > 0:
            pl.when(ten < first)(functools.partial(send, s, q))

    @pl.when(core == 1)
    def _():
        pl.semaphore_wait(barrier, total - 1)
        pl.semaphore_signal(ready, inc=1, device_id=(twin, m), device_id_type=MESH)

    @pl.when(core == 0)
    def _():
        pl.semaphore_wait(ready, 1)

    for (s, q), first in zip(SENDS, FIRST):
        if first < 4:
            pl.when(ten >= first)(functools.partial(send, s, q))

    @pl.loop(0, con.shape[0])
    def _(s):
        con[s, 9:11] = jnp.zeros((2, *con.shape[2:]), F32)

    def transform(s):
        @pl.loop(0, rows)
        def _(i):
            cs = []
            for half in range(2):
                cs += contrasts([raw[s * tms + 2 * y + half, i] for y in range(tms // 2)])
            for g in range(3):
                for k in range(3):
                    con[s, 3 * g + k, i, 0:mons] = cs[4 * g + k]
                    con[s, 3 * g + k, i, mons:8] = cs[4 * g + 3][2 * k:2 * k + 2]
            for k in range(2):
                con[s, 9 + k, i, 0:mons] = cs[12 + k]

    lane_row = lax.broadcasted_iota(jnp.int32, (8, 128), 0)

    def block(s, s2):
        cols = [jnp.zeros((8, 128), F32) for _ in range(rows)]
        for base in range(0, rows, 3):
            acc = [[None] * rows for _ in range(3)]
            for q in range(11):
                left = [con[s, q, base + a] for a in range(3)]
                right = [con[s2, q, b] for b in range(rows)]
                for a in range(3):
                    for b in range(rows):
                        prod = left[a] * right[b]
                        acc[a][b] = prod if q == 0 else acc[a][b] + prod
            for a in range(3):
                line = jnp.zeros((8, 128), F32)
                for b in range(rows):
                    r = jnp.sum(acc[a][b], axis=0, keepdims=True) * scale
                    r = jnp.broadcast_to(r, (8, 128))
                    line = jnp.where(lane_row == b, r, line)
                    cols[b] = jnp.where(lane_row == base + a, r, cols[b])
                blk[s, s2, base + a] = line[0:rows]
        for b in range(rows):
            blk[s2, s, b] = cols[b][0:rows]

    def pack(s):
        r3, r4, r5 = (blk[s, s, i] for i in range(3, 6))
        blk[s, s, 3] = jnp.concatenate([r3[3:6], r4[4:6], r5[5:6]], axis=0)

    def unpack(o):
        top = [got[o, m * rows + i] for i in range(3)]
        low = got[o, m * rows + 3]
        for i, rest in ((3, [low[0:3]]), (4, [low[1:2], low[3:5]]), (5, [low[2:3], low[4:6]])):
            got[o, m * rows + i] = jnp.concatenate([r[i:i + 1] for r in top] + rest, axis=0)

    def ship(a, b):
        if a == SELF:
            return
        lines = 4 if a == b else rows
        pltpu.make_async_remote_copy(
            src_ref=blk.at[a, b, pl.ds(0, lines)],
            dst_ref=got.at[m, pl.ds(from_m[b] * rows, lines)],
            send_sem=send3,
            recv_sem=recv3.at[m],
            device_id=(t, from_m[a]),
            device_id_type=MESH,
        ).start()

    pending = []
    for s in range(len(ORDER)):
        if s == SELF:
            mine.wait()
        n = tms - 1 if s == SELF else tms
        landed = raw.at[pl.ds(s * tms, n)]
        pltpu.make_async_remote_copy(
            src_ref=landed, dst_ref=landed, send_sem=send1, recv_sem=recv1.at[s],
            device_id=(t, m), device_id_type=MESH,
        ).wait_recv()
        transform(s)
        step = 4
        for lo in range(0, s + 1, step):
            hi = min(lo + step, s + 1)

            @pl.loop(lo, hi)
            def _(s2, s=s):
                block(s, s2)

            if hi == s + 1 and s != SELF:
                pack(s)
            for a, b in pending:
                ship(a, b)
            pending = []
            for s2 in range(lo, hi):
                pending.append((s, s2))
                if s2 != s:
                    pending.append((s2, s))
    for a, b in pending:
        ship(a, b)
    def place(o, line):
        lanes = pixels(o)

        @pl.loop(0, rows)
        def _(i):
            for n in range(members):
                out[i, n * rows:(n + 1) * rows, lanes] = line(n, i)

    for b in range(len(ORDER)):
        got[m, pl.ds(from_m[b] * rows, rows)] = blk[SELF, b]
    for o in [m] + [from_m[b] for b in range(len(ORDER)) if b != SELF]:
        if o is not m:
            part = got.at[o, pl.ds(0, members * rows - 2)]
            pltpu.make_async_remote_copy(
                src_ref=part, dst_ref=part, send_sem=send3, recv_sem=recv3.at[o],
                device_id=(t, m), device_id_type=MESH,
            ).wait_recv()
            unpack(o)
        place(o, lambda n, i, o=o: got[o, n * rows + i])

    shipped = got.at[pl.ds(0, members - 1), pl.ds(0, members * rows - 2)]
    pltpu.make_async_remote_copy(
        src_ref=shipped, dst_ref=shipped, send_sem=send3, recv_sem=recv3.at[0],
        device_id=(t, m), device_id_type=MESH,
    ).wait_send()
    sent = raw.at[pl.ds(0, total - 1)]
    pltpu.make_async_remote_copy(
        src_ref=sent, dst_ref=sent, send_sem=send1, recv_sem=recv1.at[0],
        device_id=(t, m), device_id_type=MESH,
    ).wait_send()


def per_device(fields):
    rows, mons, pixels = fields.shape
    tms, members = lax.axis_size("tm"), lax.axis_size("member")
    scale = 1.0 / (8.0 * float(mons * tms - 12))
    return pl.pallas_call(
        functools.partial(kernel, (tms, members, rows, mons, scale)),
        out_shape=jax.ShapeDtypeStruct((rows, rows * members, pixels // tms), F32),
        in_specs=[pl.BlockSpec(memory_space=pltpu.HBM)],
        out_specs=pl.BlockSpec(memory_space=pltpu.VMEM),
        scratch_shapes=[
            pltpu.VMEM((tms * members, rows, mons, 128), F32),
            pltpu.VMEM((members, 11, rows, 8, 128), F32),
            pltpu.VMEM((members, members, rows, rows, 128), F32),
            pltpu.VMEM((members, members * rows, rows, 128), F32),
            pltpu.SemaphoreType.DMA,
            pltpu.SemaphoreType.DMA((members,)),
            pltpu.SemaphoreType.DMA,
            pltpu.SemaphoreType.DMA,
            pltpu.SemaphoreType.DMA((members,)),
            pltpu.SemaphoreType.REGULAR,
        ],
        compiler_params=pltpu.CompilerParams(collective_id=0, has_side_effects=True, vmem_limit_bytes=50 * 2**20),
        name="cov",
    )(fields)


def solution(mesh):
    in_specs = (P("member", "tm", None),)
    out_specs = P("member", None, "tm")
    return jax.shard_map(per_device, mesh=mesh, in_specs=in_specs, out_specs=out_specs, check_vma=False)
```

```python
import functools

import jax
import jax.numpy as jnp
from jax import lax
from jax.experimental import pallas as pl
from jax.experimental.pallas import tpu as pltpu
from jax.sharding import PartitionSpec as P

MESH = pl.DeviceIdType.MESH
F32 = jnp.float32
ORDER = ((2, 1), (0, 0), (2, 0), (0, 1), (1, 0), (3, 1), (3, 0), (1, 1))
SELF = ORDER.index((0, 0))
SENDS = (
    (7, 3), (6, 3), (1, 3), (0, 3), (2, 3), (3, 3), (5, 3), (4, 3), (0, 8), (1, 1), (0, 9), (1, 4),
    (0, 12), (1, 12), (0, 4), (1, 13), (0, 5), (1, 9), (0, 0), (1, 8), (0, 1), (1, 5), (0, 13), (1, 10),
    (0, 2), (1, 11), (0, 6), (1, 15), (0, 11), (1, 2), (0, 10), (1, 6), (0, 15), (1, 7), (0, 14), (1, 14),
    (0, 7), (3, 9), (2, 0), (3, 11), (2, 2), (2, 8), (3, 1), (2, 11), (3, 2), (2, 9), (3, 0), (3, 10),
    (2, 7), (3, 15), (2, 6), (3, 13), (2, 13), (3, 4), (2, 4), (3, 14), (2, 10), (2, 1), (3, 8), (3, 6),
    (2, 14), (3, 5), (2, 12), (3, 12), (2, 5), (3, 7), (2, 15), (5, 9), (4, 0), (5, 11), (4, 2), (4, 8),
    (5, 1), (4, 11), (5, 2), (4, 9), (5, 0), (5, 10), (4, 7), (5, 15), (4, 6), (5, 13), (4, 13), (5, 4),
    (4, 4), (5, 14), (4, 10), (4, 1), (5, 8), (5, 6), (4, 14), (5, 5), (4, 12), (5, 12), (4, 5), (5, 7),
    (4, 15), (7, 9), (6, 0), (7, 11), (6, 2), (6, 8), (7, 1), (6, 11), (7, 2), (6, 9), (7, 0), (7, 10),
    (6, 7), (7, 15), (6, 6), (7, 13), (6, 13), (7, 4), (6, 4), (7, 14), (6, 10), (6, 1), (7, 8), (7, 6),
    (6, 14), (7, 5), (6, 12), (7, 12), (6, 5), (7, 7), (6, 15),
)
FIRST = (
    4, 4, 4, 4, 4, 4, 4, 4, 0, 0, 0, 0, 0, 0, 0, 0, 0, 0, 1, 0, 0, 0, 0, 0, 0, 0, 0, 0, 0, 0,
    0, 0, 0, 0, 0, 0, 0, 0, 1, 0, 0, 0, 0, 0, 0, 0, 0, 0, 0, 0, 0, 0, 0, 0, 0, 0, 0, 0, 0, 0,
    0, 0, 0, 0, 0, 0, 0, 0, 0, 0, 0, 0, 0, 0, 0, 0, 0, 0, 0, 0, 0, 0, 0, 0, 0, 0, 0, 0, 0, 0,
    0, 0, 0, 0, 0, 0, 0, 0, 0, 0, 0, 0, 0, 0, 0, 0, 0, 0, 0, 0, 0, 0, 0, 0, 0, 0, 0, 0, 0, 0,
    0, 0, 0, 0, 0, 0, 0,
)


def contrasts(years):
    shifted = [y - years[0] for y in years[1:]]
    a1, a2, a3, a4, a5, a6, a7 = shifted
    p0, m0 = a4, -a4
    p1, m1 = a1 + a5, a1 - a5
    p2, m2 = a2 + a6, a2 - a6
    p3, m3 = a3 + a7, a3 - a7
    out = []
    q0, q2, q1, q3 = p0 + p2, p0 - p2, p1 + p3, p1 - p3
    out += [q0 - q1, q2 + q3, q2 - q3]
    r0, r2, r1, r3 = m0 + m2, m0 - m2, m1 + m3, m1 - m3
    out += [r0 + r1, r0 - r1, r2 + r3, r2 - r3]
    return out


def kernel(sizes, fields, out, raw, con, blk, got, send1, recv1, own, send3, recv3, ready):
    tms, members, rows, mons, scale = sizes
    t, m = lax.axis_index("tm"), lax.axis_index("member")
    me = t * members + m
    total = tms * members
    x, h = m // 2, m % 2
    ten, low, core = t // 4, (t // 2) % 2, t % 2

    barrier = pltpu.get_barrier_semaphore()

    near_t = [((ten + q // 4) % 4) * 4 + ((low + (q // 2) % 2) % 2) * 2 + (core + q % 2) % 2 for q in range(tms)]
    from_m = [((x + dx) % 4) * 2 + (h + dh) % 2 for dx, dh in ORDER]
    to_m = [((x + 4 - dx) % 4) * 2 + (h + dh) % 2 for dx, dh in ORDER]

    def greet(other_t, other_m):
        pl.semaphore_signal(barrier, inc=1, device_id=(other_t, other_m), device_id_type=MESH)

    twin = t + 1 - 2 * core
    for s in range(len(ORDER)):
        for q in range(0, 4, 2):
            seen = near_t[q] - core
            if s == SELF and q == 0:
                pl.when(core == 1)(functools.partial(greet, seen, m))
            else:
                greet(seen, to_m[s])
    for s in range(len(ORDER)):
        for q in range(0, tms, 2):
            seen = near_t[q] + 1 - core
            if s == SELF and q == 0:
                pl.when(core == 0)(functools.partial(greet, seen, m))
            else:
                greet(seen, to_m[s])

    def pixels(d):
        return pl.ds(pl.multiple_of(d * 128, 128), 128)

    mine = pltpu.make_async_copy(fields.at[:, :, pixels(me)], raw.at[SELF * tms + t], own)
    mine.start()

    def send(s, q):
        pltpu.make_async_remote_copy(
            src_ref=fields.at[:, :, pixels(near_t[q] * members + to_m[s])],
            dst_ref=raw.at[s * tms + t],
            send_sem=send1,
            recv_sem=recv1.at[s],
            device_id=(near_t[q], to_m[s]),
            device_id_type=MESH,
        ).start()

    @pl.when(core == 0)
    def _():
        pl.semaphore_wait(barrier, 4 * members - 1)
        pl.semaphore_signal(ready, inc=1, device_id=(twin, m), device_id_type=MESH)

    @pl.when(core == 1)
    def _():
        pl.semaphore_wait(ready, 1)

    for (s, q), first in zip(SENDS, FIRST):
        if first > 0:
            pl.when(ten < first)(functools.partial(send, s, q))

    @pl.when(core == 1)
    def _():
        pl.semaphore_wait(barrier, total - 1)
        pl.semaphore_signal(ready, inc=1, device_id=(twin, m), device_id_type=MESH)

    @pl.when(core == 0)
    def _():
        pl.semaphore_wait(ready, 1)

    for (s, q), first in zip(SENDS, FIRST):
        if first < 4:
            pl.when(ten >= first)(functools.partial(send, s, q))

    @pl.loop(0, con.shape[0])
    def _(s):
        con[s, 9:11] = jnp.zeros((2, *con.shape[2:]), F32)

    def transform(s):
        @pl.loop(0, rows)
        def _(i):
            cs = []
            for half in range(2):
                cs += contrasts([raw[s * tms + 2 * y + half, i] for y in range(tms // 2)])
            for g in range(3):
                for k in range(3):
                    con[s, 3 * g + k, i, 0:mons] = cs[4 * g + k]
                    con[s, 3 * g + k, i, mons:8] = cs[4 * g + 3][2 * k:2 * k + 2]
            for k in range(2):
                con[s, 9 + k, i, 0:mons] = cs[12 + k]

    lane_row = lax.broadcasted_iota(jnp.int32, (8, 128), 0)

    def block(s, s2):
        cols = [jnp.zeros((8, 128), F32) for _ in range(rows)]
        for base in range(0, rows, 3):
            acc = [[None] * rows for _ in range(3)]
            for q in range(11):
                left = [con[s, q, base + a] for a in range(3)]
                right = [con[s2, q, b] for b in range(rows)]
                for a in range(3):
                    for b in range(rows):
                        prod = left[a] * right[b]
                        acc[a][b] = prod if q == 0 else acc[a][b] + prod
            for a in range(3):
                line = jnp.zeros((8, 128), F32)
                for b in range(rows):
                    r = jnp.sum(acc[a][b], axis=0, keepdims=True) * scale
                    r = jnp.broadcast_to(r, (8, 128))
                    line = jnp.where(lane_row == b, r, line)
                    cols[b] = jnp.where(lane_row == base + a, r, cols[b])
                blk[s, s2, base + a] = line[0:rows]
        for b in range(rows):
            blk[s2, s, b] = cols[b][0:rows]

    def pack(s):
        r3, r4, r5 = (blk[s, s, i] for i in range(3, 6))
        blk[s, s, 3] = jnp.concatenate([r3[3:6], r4[4:6], r5[5:6]], axis=0)

    def unpack(o):
        top = [got[o, m * rows + i] for i in range(3)]
        low = got[o, m * rows + 3]
        for i, rest in ((3, [low[0:3]]), (4, [low[1:2], low[3:5]]), (5, [low[2:3], low[4:6]])):
            got[o, m * rows + i] = jnp.concatenate([r[i:i + 1] for r in top] + rest, axis=0)

    def ship(a, b):
        if a == SELF:
            return
        lines = 4 if a == b else rows
        pltpu.make_async_remote_copy(
            src_ref=blk.at[a, b, pl.ds(0, lines)],
            dst_ref=got.at[m, pl.ds(from_m[b] * rows, lines)],
            send_sem=send3,
            recv_sem=recv3.at[m],
            device_id=(t, from_m[a]),
            device_id_type=MESH,
        ).start()

    pending = []
    for s in range(len(ORDER)):
        if s == SELF:
            mine.wait()
        n = tms - 1 if s == SELF else tms
        landed = raw.at[pl.ds(s * tms, n)]
        pltpu.make_async_remote_copy(
            src_ref=landed, dst_ref=landed, send_sem=send1, recv_sem=recv1.at[s],
            device_id=(t, m), device_id_type=MESH,
        ).wait_recv()
        transform(s)
        step = 3
        for lo in range(0, s + 1, step):
            hi = min(lo + step, s + 1)

            @pl.loop(lo, hi)
            def _(s2, s=s):
                block(s, s2)

            if hi == s + 1 and s != SELF:
                pack(s)
            for a, b in pending:
                ship(a, b)
            pending = []
            for s2 in range(lo, hi):
                pending.append((s, s2))
                if s2 != s:
                    pending.append((s2, s))
    for a, b in pending:
        ship(a, b)
    def place(o, line):
        lanes = pixels(o)

        @pl.loop(0, rows)
        def _(i):
            for n in range(members):
                out[i, n * rows:(n + 1) * rows, lanes] = line(n, i)

    for b in range(len(ORDER)):
        got[m, pl.ds(from_m[b] * rows, rows)] = blk[SELF, b]
    for o in [m] + [from_m[b] for b in range(len(ORDER)) if b != SELF]:
        if o is not m:
            part = got.at[o, pl.ds(0, members * rows - 2)]
            pltpu.make_async_remote_copy(
                src_ref=part, dst_ref=part, send_sem=send3, recv_sem=recv3.at[o],
                device_id=(t, m), device_id_type=MESH,
            ).wait_recv()
            unpack(o)
        place(o, lambda n, i, o=o: got[o, n * rows + i])

    shipped = got.at[pl.ds(0, members - 1), pl.ds(0, members * rows - 2)]
    pltpu.make_async_remote_copy(
        src_ref=shipped, dst_ref=shipped, send_sem=send3, recv_sem=recv3.at[0],
        device_id=(t, m), device_id_type=MESH,
    ).wait_send()
    sent = raw.at[pl.ds(0, total - 1)]
    pltpu.make_async_remote_copy(
        src_ref=sent, dst_ref=sent, send_sem=send1, recv_sem=recv1.at[0],
        device_id=(t, m), device_id_type=MESH,
    ).wait_send()


def per_device(fields):
    rows, mons, pixels = fields.shape
    tms, members = lax.axis_size("tm"), lax.axis_size("member")
    scale = 1.0 / (8.0 * float(mons * tms - 12))
    return pl.pallas_call(
        functools.partial(kernel, (tms, members, rows, mons, scale)),
        out_shape=jax.ShapeDtypeStruct((rows, rows * members, pixels // tms), F32),
        in_specs=[pl.BlockSpec(memory_space=pltpu.HBM)],
        out_specs=pl.BlockSpec(memory_space=pltpu.VMEM),
        scratch_shapes=[
            pltpu.VMEM((tms * members, rows, mons, 128), F32),
            pltpu.VMEM((members, 11, rows, 8, 128), F32),
            pltpu.VMEM((members, members, rows, rows, 128), F32),
            pltpu.VMEM((members, members * rows, rows, 128), F32),
            pltpu.SemaphoreType.DMA,
            pltpu.SemaphoreType.DMA((members,)),
            pltpu.SemaphoreType.DMA,
            pltpu.SemaphoreType.DMA,
            pltpu.SemaphoreType.DMA((members,)),
            pltpu.SemaphoreType.REGULAR,
        ],
        compiler_params=pltpu.CompilerParams(collective_id=0, has_side_effects=True, vmem_limit_bytes=50 * 2**20),
        name="cov",
    )(fields)


def solution(mesh):
    in_specs = (P("member", "tm", None),)
    out_specs = P("member", None, "tm")
    return jax.shard_map(per_device, mesh=mesh, in_specs=in_specs, out_specs=out_specs, check_vma=False)
```

```python
import functools

import jax
import jax.numpy as jnp
from jax import lax
from jax.experimental import pallas as pl
from jax.experimental.pallas import tpu as pltpu
from jax.sharding import PartitionSpec as P

MESH = pl.DeviceIdType.MESH
F32 = jnp.float32
ORDER = ((2, 1), (0, 0), (2, 0), (0, 1), (1, 0), (3, 1), (3, 0), (1, 1))
SELF = ORDER.index((0, 0))
SENDS = (
    (7, 3), (6, 3), (1, 3), (0, 3), (2, 3), (3, 3), (5, 3), (4, 3), (0, 8), (1, 1), (0, 9), (1, 4),
    (0, 12), (1, 12), (0, 4), (1, 13), (0, 5), (1, 9), (0, 0), (1, 8), (0, 1), (1, 5), (0, 13), (1, 10),
    (0, 2), (1, 11), (0, 6), (1, 15), (0, 11), (1, 2), (0, 10), (1, 6), (0, 15), (1, 7), (0, 14), (1, 14),
    (0, 7), (3, 9), (2, 0), (3, 11), (2, 2), (2, 8), (3, 1), (2, 11), (3, 2), (2, 9), (3, 0), (3, 10),
    (2, 7), (3, 15), (2, 6), (3, 13), (2, 13), (3, 4), (2, 4), (3, 14), (2, 10), (2, 1), (3, 8), (3, 6),
    (2, 14), (3, 5), (2, 12), (3, 12), (2, 5), (3, 7), (2, 15), (5, 9), (4, 0), (5, 11), (4, 2), (4, 8),
    (5, 1), (4, 11), (5, 2), (4, 9), (5, 0), (5, 10), (4, 7), (5, 15), (4, 6), (5, 13), (4, 13), (5, 4),
    (4, 4), (5, 14), (4, 10), (4, 1), (5, 8), (5, 6), (4, 14), (5, 5), (4, 12), (5, 12), (4, 5), (5, 7),
    (4, 15), (7, 9), (6, 0), (7, 11), (6, 2), (6, 8), (7, 1), (6, 11), (7, 2), (6, 9), (7, 0), (7, 10),
    (6, 7), (7, 15), (6, 6), (7, 13), (6, 13), (7, 4), (6, 4), (7, 14), (6, 10), (6, 1), (7, 8), (7, 6),
    (6, 14), (7, 5), (6, 12), (7, 12), (6, 5), (7, 7), (6, 15),
)
FIRST = (
    4, 4, 4, 4, 4, 4, 4, 4, 0, 0, 0, 0, 0, 0, 0, 0, 0, 0, 0, 0, 1, 0, 0, 0, 0, 0, 0, 0, 0, 0,
    0, 0, 0, 0, 0, 0, 0, 0, 0, 0, 0, 0, 0, 0, 0, 0, 0, 0, 0, 0, 0, 0, 0, 0, 0, 0, 0, 1, 0, 0,
    0, 0, 0, 0, 0, 0, 0, 0, 0, 0, 0, 0, 0, 0, 0, 0, 0, 0, 0, 0, 0, 0, 0, 0, 0, 0, 0, 0, 0, 0,
    0, 0, 0, 0, 0, 0, 0, 0, 0, 0, 0, 0, 0, 0, 0, 0, 0, 0, 0, 0, 0, 0, 0, 0, 0, 0, 0, 0, 0, 0,
    0, 0, 0, 0, 0, 0, 0,
)


def contrasts(years):
    shifted = [y - years[0] for y in years[1:]]
    a1, a2, a3, a4, a5, a6, a7 = shifted
    p0, m0 = a4, -a4
    p1, m1 = a1 + a5, a1 - a5
    p2, m2 = a2 + a6, a2 - a6
    p3, m3 = a3 + a7, a3 - a7
    out = []
    q0, q2, q1, q3 = p0 + p2, p0 - p2, p1 + p3, p1 - p3
    out += [q0 - q1, q2 + q3, q2 - q3]
    r0, r2, r1, r3 = m0 + m2, m0 - m2, m1 + m3, m1 - m3
    out += [r0 + r1, r0 - r1, r2 + r3, r2 - r3]
    return out


def kernel(sizes, fields, out, raw, con, blk, got, send1, recv1, own, send3, recv3, ready):
    tms, members, rows, mons, scale = sizes
    t, m = lax.axis_index("tm"), lax.axis_index("member")
    me = t * members + m
    total = tms * members
    x, h = m // 2, m % 2
    ten, low, core = t // 4, (t // 2) % 2, t % 2

    barrier = pltpu.get_barrier_semaphore()

    near_t = [((ten + q // 4) % 4) * 4 + ((low + (q // 2) % 2) % 2) * 2 + (core + q % 2) % 2 for q in range(tms)]
    from_m = [((x + dx) % 4) * 2 + (h + dh) % 2 for dx, dh in ORDER]
    to_m = [((x + 4 - dx) % 4) * 2 + (h + dh) % 2 for dx, dh in ORDER]

    def greet(other_t, other_m):
        pl.semaphore_signal(barrier, inc=1, device_id=(other_t, other_m), device_id_type=MESH)

    twin = t + 1 - 2 * core
    for s in range(len(ORDER)):
        for q in range(0, 4, 2):
            seen = near_t[q] - core
            if s == SELF and q == 0:
                pl.when(core == 1)(functools.partial(greet, seen, m))
            else:
                greet(seen, to_m[s])
    for s in range(len(ORDER)):
        for q in range(0, tms, 2):
            seen = near_t[q] + 1 - core
            if s == SELF and q == 0:
                pl.when(core == 0)(functools.partial(greet, seen, m))
            else:
                greet(seen, to_m[s])

    def pixels(d):
        return pl.ds(pl.multiple_of(d * 128, 128), 128)

    mine = pltpu.make_async_copy(fields.at[:, :, pixels(me)], raw.at[SELF * tms + t], own)
    mine.start()

    def send(s, q):
        pltpu.make_async_remote_copy(
            src_ref=fields.at[:, :, pixels(near_t[q] * members + to_m[s])],
            dst_ref=raw.at[s * tms + t],
            send_sem=send1,
            recv_sem=recv1.at[s],
            device_id=(near_t[q], to_m[s]),
            device_id_type=MESH,
        ).start()

    @pl.when(core == 0)
    def _():
        pl.semaphore_wait(barrier, 4 * members - 1)
        pl.semaphore_signal(ready, inc=1, device_id=(twin, m), device_id_type=MESH)

    @pl.when(core == 1)
    def _():
        pl.semaphore_wait(ready, 1)

    for (s, q), first in zip(SENDS, FIRST):
        if first > 0:
            pl.when(ten < first)(functools.partial(send, s, q))

    @pl.when(core == 1)
    def _():
        pl.semaphore_wait(barrier, total - 1)
        pl.semaphore_signal(ready, inc=1, device_id=(twin, m), device_id_type=MESH)

    @pl.when(core == 0)
    def _():
        pl.semaphore_wait(ready, 1)

    for (s, q), first in zip(SENDS, FIRST):
        if first < 4:
            pl.when(ten >= first)(functools.partial(send, s, q))

    @pl.loop(0, con.shape[0])
    def _(s):
        con[s, 9:11] = jnp.zeros((2, *con.shape[2:]), F32)

    def transform(s):
        @pl.loop(0, rows)
        def _(i):
            cs = []
            for half in range(2):
                cs += contrasts([raw[s * tms + 2 * y + half, i] for y in range(tms // 2)])
            for g in range(3):
                for k in range(3):
                    con[s, 3 * g + k, i, 0:mons] = cs[4 * g + k]
                    con[s, 3 * g + k, i, mons:8] = cs[4 * g + 3][2 * k:2 * k + 2]
            for k in range(2):
                con[s, 9 + k, i, 0:mons] = cs[12 + k]

    lane_row = lax.broadcasted_iota(jnp.int32, (8, 128), 0)

    def block(s, s2):
        cols = [jnp.zeros((8, 128), F32) for _ in range(rows)]
        for base in range(0, rows, 3):
            acc = [[None] * rows for _ in range(3)]
            for q in range(11):
                left = [con[s, q, base + a] for a in range(3)]
                right = [con[s2, q, b] for b in range(rows)]
                for a in range(3):
                    for b in range(rows):
                        prod = left[a] * right[b]
                        acc[a][b] = prod if q == 0 else acc[a][b] + prod
            for a in range(3):
                line = jnp.zeros((8, 128), F32)
                for b in range(rows):
                    r = jnp.sum(acc[a][b], axis=0, keepdims=True) * scale
                    r = jnp.broadcast_to(r, (8, 128))
                    line = jnp.where(lane_row == b, r, line)
                    cols[b] = jnp.where(lane_row == base + a, r, cols[b])
                blk[s, s2, base + a] = line[0:rows]
        for b in range(rows):
            blk[s2, s, b] = cols[b][0:rows]

    def pack(s):
        r3, r4, r5 = (blk[s, s, i] for i in range(3, 6))
        blk[s, s, 3] = jnp.concatenate([r3[3:6], r4[4:6], r5[5:6]], axis=0)

    def unpack(o):
        top = [got[o, m * rows + i] for i in range(3)]
        low = got[o, m * rows + 3]
        for i, rest in ((3, [low[0:3]]), (4, [low[1:2], low[3:5]]), (5, [low[2:3], low[4:6]])):
            got[o, m * rows + i] = jnp.concatenate([r[i:i + 1] for r in top] + rest, axis=0)

    def ship(a, b):
        if a == SELF:
            return
        lines = 4 if a == b else rows
        pltpu.make_async_remote_copy(
            src_ref=blk.at[a, b, pl.ds(0, lines)],
            dst_ref=got.at[m, pl.ds(from_m[b] * rows, lines)],
            send_sem=send3,
            recv_sem=recv3.at[m],
            device_id=(t, from_m[a]),
            device_id_type=MESH,
        ).start()

    pending = []
    for s in range(len(ORDER)):
        if s == SELF:
            mine.wait()
        n = tms - 1 if s == SELF else tms
        landed = raw.at[pl.ds(s * tms, n)]
        pltpu.make_async_remote_copy(
            src_ref=landed, dst_ref=landed, send_sem=send1, recv_sem=recv1.at[s],
            device_id=(t, m), device_id_type=MESH,
        ).wait_recv()
        transform(s)
        step = 3
        for lo in range(0, s + 1, step):
            hi = min(lo + step, s + 1)

            @pl.loop(lo, hi)
            def _(s2, s=s):
                block(s, s2)

            if hi == s + 1 and s != SELF:
                pack(s)
            for a, b in pending:
                ship(a, b)
            pending = []
            for s2 in range(lo, hi):
                pending.append((s, s2))
                if s2 != s:
                    pending.append((s2, s))
    for a, b in pending:
        ship(a, b)
    def place(o, line):
        lanes = pixels(o)

        @pl.loop(0, rows)
        def _(i):
            for n in range(members):
                out[i, n * rows:(n + 1) * rows, lanes] = line(n, i)

    for b in range(len(ORDER)):
        got[m, pl.ds(from_m[b] * rows, rows)] = blk[SELF, b]
    for o in [m] + [from_m[b] for b in range(len(ORDER)) if b != SELF]:
        if o is not m:
            part = got.at[o, pl.ds(0, members * rows - 2)]
            pltpu.make_async_remote_copy(
                src_ref=part, dst_ref=part, send_sem=send3, recv_sem=recv3.at[o],
                device_id=(t, m), device_id_type=MESH,
            ).wait_recv()
            unpack(o)
        place(o, lambda n, i, o=o: got[o, n * rows + i])

    shipped = got.at[pl.ds(0, members - 1), pl.ds(0, members * rows - 2)]
    pltpu.make_async_remote_copy(
        src_ref=shipped, dst_ref=shipped, send_sem=send3, recv_sem=recv3.at[0],
        device_id=(t, m), device_id_type=MESH,
    ).wait_send()
    sent = raw.at[pl.ds(0, total - 1)]
    pltpu.make_async_remote_copy(
        src_ref=sent, dst_ref=sent, send_sem=send1, recv_sem=recv1.at[0],
        device_id=(t, m), device_id_type=MESH,
    ).wait_send()


def per_device(fields):
    rows, mons, pixels = fields.shape
    tms, members = lax.axis_size("tm"), lax.axis_size("member")
    scale = 1.0 / (8.0 * float(mons * tms - 12))
    return pl.pallas_call(
        functools.partial(kernel, (tms, members, rows, mons, scale)),
        out_shape=jax.ShapeDtypeStruct((rows, rows * members, pixels // tms), F32),
        in_specs=[pl.BlockSpec(memory_space=pltpu.HBM)],
        out_specs=pl.BlockSpec(memory_space=pltpu.VMEM),
        scratch_shapes=[
            pltpu.VMEM((tms * members, rows, mons, 128), F32),
            pltpu.VMEM((members, 11, rows, 8, 128), F32),
            pltpu.VMEM((members, members, rows, rows, 128), F32),
            pltpu.VMEM((members, members * rows, rows, 128), F32),
            pltpu.SemaphoreType.DMA,
            pltpu.SemaphoreType.DMA((members,)),
            pltpu.SemaphoreType.DMA,
            pltpu.SemaphoreType.DMA,
            pltpu.SemaphoreType.DMA((members,)),
            pltpu.SemaphoreType.REGULAR,
        ],
        compiler_params=pltpu.CompilerParams(collective_id=0, has_side_effects=True, vmem_limit_bytes=50 * 2**20),
        name="cov",
    )(fields)


def solution(mesh):
    in_specs = (P("member", "tm", None),)
    out_specs = P("member", None, "tm")
    return jax.shard_map(per_device, mesh=mesh, in_specs=in_specs, out_specs=out_specs, check_vma=False)
```

```python
import functools

import jax
import jax.numpy as jnp
from jax import lax
from jax.experimental import pallas as pl
from jax.experimental.pallas import tpu as pltpu
from jax.sharding import PartitionSpec as P

MESH = pl.DeviceIdType.MESH
F32 = jnp.float32
ORDER = ((2, 1), (0, 0), (2, 0), (0, 1), (1, 0), (3, 1), (3, 0), (1, 1))
SELF = ORDER.index((0, 0))
SENDS = (
    (7, 3), (6, 3), (1, 3), (0, 3), (2, 3), (3, 3), (5, 3), (4, 3), (0, 8), (1, 1), (0, 9), (1, 4),
    (0, 12), (1, 12), (0, 4), (1, 13), (0, 5), (1, 9), (0, 0), (1, 8), (0, 1), (1, 5), (0, 13), (1, 10),
    (0, 2), (1, 11), (0, 6), (1, 15), (0, 11), (1, 2), (0, 10), (1, 6), (0, 15), (1, 7), (0, 14), (1, 14),
    (0, 7), (3, 9), (2, 0), (3, 11), (2, 2), (2, 8), (3, 1), (2, 11), (3, 2), (2, 9), (3, 0), (3, 10),
    (2, 7), (3, 15), (2, 6), (3, 13), (2, 13), (3, 4), (2, 4), (3, 14), (2, 10), (2, 1), (3, 8), (3, 6),
    (2, 14), (3, 5), (2, 12), (3, 12), (2, 5), (3, 7), (2, 15), (5, 9), (4, 0), (5, 11), (4, 2), (4, 8),
    (5, 1), (4, 11), (5, 2), (4, 9), (5, 0), (5, 10), (4, 7), (5, 15), (4, 6), (5, 13), (4, 13), (5, 4),
    (4, 4), (5, 14), (4, 10), (4, 1), (5, 8), (5, 6), (4, 14), (5, 5), (4, 12), (5, 12), (4, 5), (5, 7),
    (4, 15), (7, 9), (6, 0), (7, 11), (6, 2), (6, 8), (7, 1), (6, 11), (7, 2), (6, 9), (7, 0), (7, 10),
    (6, 7), (7, 15), (6, 6), (7, 13), (6, 13), (7, 4), (6, 4), (7, 14), (6, 10), (6, 1), (7, 8), (7, 6),
    (6, 14), (7, 5), (6, 12), (7, 12), (6, 5), (7, 7), (6, 15),
)
FIRST = (
    4, 4, 4, 4, 4, 4, 4, 4, 0, 0, 0, 0, 0, 0, 0, 0, 0, 0, 0, 0, 1, 0, 0, 0, 0, 0, 0, 0, 0, 0,
    0, 0, 0, 0, 0, 0, 0, 0, 0, 0, 0, 0, 0, 0, 1, 0, 0, 0, 0, 0, 0, 0, 0, 0, 0, 0, 0, 1, 0, 0,
    0, 0, 0, 0, 0, 0, 0, 0, 0, 0, 0, 0, 0, 0, 0, 0, 0, 0, 0, 0, 0, 0, 0, 0, 0, 0, 0, 0, 0, 0,
    0, 0, 0, 0, 0, 0, 0, 0, 0, 0, 0, 0, 0, 0, 0, 0, 0, 0, 0, 0, 0, 0, 0, 0, 0, 0, 0, 0, 0, 0,
    0, 0, 0, 0, 0, 0, 0,
)


def contrasts(years):
    shifted = [y - years[0] for y in years[1:]]
    a1, a2, a3, a4, a5, a6, a7 = shifted
    p0, m0 = a4, -a4
    p1, m1 = a1 + a5, a1 - a5
    p2, m2 = a2 + a6, a2 - a6
    p3, m3 = a3 + a7, a3 - a7
    out = []
    q0, q2, q1, q3 = p0 + p2, p0 - p2, p1 + p3, p1 - p3
    out += [q0 - q1, q2 + q3, q2 - q3]
    r0, r2, r1, r3 = m0 + m2, m0 - m2, m1 + m3, m1 - m3
    out += [r0 + r1, r0 - r1, r2 + r3, r2 - r3]
    return out


def kernel(sizes, fields, out, raw, con, blk, got, send1, recv1, own, send3, recv3, ready):
    tms, members, rows, mons, scale = sizes
    t, m = lax.axis_index("tm"), lax.axis_index("member")
    me = t * members + m
    total = tms * members
    x, h = m // 2, m % 2
    ten, low, core = t // 4, (t // 2) % 2, t % 2

    barrier = pltpu.get_barrier_semaphore()

    near_t = [((ten + q // 4) % 4) * 4 + ((low + (q // 2) % 2) % 2) * 2 + (core + q % 2) % 2 for q in range(tms)]
    from_m = [((x + dx) % 4) * 2 + (h + dh) % 2 for dx, dh in ORDER]
    to_m = [((x + 4 - dx) % 4) * 2 + (h + dh) % 2 for dx, dh in ORDER]

    def greet(other_t, other_m):
        pl.semaphore_signal(barrier, inc=1, device_id=(other_t, other_m), device_id_type=MESH)

    twin = t + 1 - 2 * core
    for s in range(len(ORDER)):
        for q in range(0, 4, 2):
            seen = near_t[q] - core
            if s == SELF and q == 0:
                pl.when(core == 1)(functools.partial(greet, seen, m))
            else:
                greet(seen, to_m[s])
    for s in range(len(ORDER)):
        for q in range(0, tms, 2):
            seen = near_t[q] + 1 - core
            if s == SELF and q == 0:
                pl.when(core == 0)(functools.partial(greet, seen, m))
            else:
                greet(seen, to_m[s])

    def pixels(d):
        return pl.ds(pl.multiple_of(d * 128, 128), 128)

    mine = pltpu.make_async_copy(fields.at[:, :, pixels(me)], raw.at[SELF * tms + t], own)
    mine.start()

    def send(s, q):
        pltpu.make_async_remote_copy(
            src_ref=fields.at[:, :, pixels(near_t[q] * members + to_m[s])],
            dst_ref=raw.at[s * tms + t],
            send_sem=send1,
            recv_sem=recv1.at[s],
            device_id=(near_t[q], to_m[s]),
            device_id_type=MESH,
        ).start()

    @pl.when(core == 0)
    def _():
        pl.semaphore_wait(barrier, 4 * members - 1)
        pl.semaphore_signal(ready, inc=1, device_id=(twin, m), device_id_type=MESH)

    @pl.when(core == 1)
    def _():
        pl.semaphore_wait(ready, 1)

    for (s, q), first in zip(SENDS, FIRST):
        if first > 0:
            pl.when(ten < first)(functools.partial(send, s, q))

    @pl.when(core == 1)
    def _():
        pl.semaphore_wait(barrier, total - 1)
        pl.semaphore_signal(ready, inc=1, device_id=(twin, m), device_id_type=MESH)

    @pl.when(core == 0)
    def _():
        pl.semaphore_wait(ready, 1)

    for (s, q), first in zip(SENDS, FIRST):
        if first < 4:
            pl.when(ten >= first)(functools.partial(send, s, q))

    @pl.loop(0, con.shape[0])
    def _(s):
        con[s, 9:11] = jnp.zeros((2, *con.shape[2:]), F32)

    def transform(s):
        @pl.loop(0, rows)
        def _(i):
            cs = []
            for half in range(2):
                cs += contrasts([raw[s * tms + 2 * y + half, i] for y in range(tms // 2)])
            for g in range(3):
                for k in range(3):
                    con[s, 3 * g + k, i, 0:mons] = cs[4 * g + k]
                    con[s, 3 * g + k, i, mons:8] = cs[4 * g + 3][2 * k:2 * k + 2]
            for k in range(2):
                con[s, 9 + k, i, 0:mons] = cs[12 + k]

    lane_row = lax.broadcasted_iota(jnp.int32, (8, 128), 0)

    def block(s, s2):
        cols = [jnp.zeros((8, 128), F32) for _ in range(rows)]
        for base in range(0, rows, 3):
            acc = [[None] * rows for _ in range(3)]
            for q in range(11):
                left = [con[s, q, base + a] for a in range(3)]
                right = [con[s2, q, b] for b in range(rows)]
                for a in range(3):
                    for b in range(rows):
                        prod = left[a] * right[b]
                        acc[a][b] = prod if q == 0 else acc[a][b] + prod
            for a in range(3):
                line = jnp.zeros((8, 128), F32)
                for b in range(rows):
                    r = jnp.sum(acc[a][b], axis=0, keepdims=True) * scale
                    r = jnp.broadcast_to(r, (8, 128))
                    line = jnp.where(lane_row == b, r, line)
                    cols[b] = jnp.where(lane_row == base + a, r, cols[b])
                blk[s, s2, base + a] = line[0:rows]
        for b in range(rows):
            blk[s2, s, b] = cols[b][0:rows]

    def pack(s):
        r3, r4, r5 = (blk[s, s, i] for i in range(3, 6))
        blk[s, s, 3] = jnp.concatenate([r3[3:6], r4[4:6], r5[5:6]], axis=0)

    def unpack(o):
        top = [got[o, m * rows + i] for i in range(3)]
        low = got[o, m * rows + 3]
        for i, rest in ((3, [low[0:3]]), (4, [low[1:2], low[3:5]]), (5, [low[2:3], low[4:6]])):
            got[o, m * rows + i] = jnp.concatenate([r[i:i + 1] for r in top] + rest, axis=0)

    def ship(a, b):
        if a == SELF:
            return
        lines = 4 if a == b else rows
        pltpu.make_async_remote_copy(
            src_ref=blk.at[a, b, pl.ds(0, lines)],
            dst_ref=got.at[m, pl.ds(from_m[b] * rows, lines)],
            send_sem=send3,
            recv_sem=recv3.at[m],
            device_id=(t, from_m[a]),
            device_id_type=MESH,
        ).start()

    pending = []
    for s in range(len(ORDER)):
        if s == SELF:
            mine.wait()
        n = tms - 1 if s == SELF else tms
        landed = raw.at[pl.ds(s * tms, n)]
        pltpu.make_async_remote_copy(
            src_ref=landed, dst_ref=landed, send_sem=send1, recv_sem=recv1.at[s],
            device_id=(t, m), device_id_type=MESH,
        ).wait_recv()
        transform(s)
        step = 3
        for lo in range(0, s + 1, step):
            hi = min(lo + step, s + 1)

            @pl.loop(lo, hi)
            def _(s2, s=s):
                block(s, s2)

            if hi == s + 1 and s != SELF:
                pack(s)
            for a, b in pending:
                ship(a, b)
            pending = []
            for s2 in range(lo, hi):
                pending.append((s, s2))
                if s2 != s:
                    pending.append((s2, s))
    for a, b in pending:
        ship(a, b)
    def place(o, line):
        lanes = pixels(o)

        @pl.loop(0, rows)
        def _(i):
            for n in range(members):
                out[i, n * rows:(n + 1) * rows, lanes] = line(n, i)

    for b in range(len(ORDER)):
        got[m, pl.ds(from_m[b] * rows, rows)] = blk[SELF, b]
    for o in [m] + [from_m[b] for b in range(len(ORDER)) if b != SELF]:
        if o is not m:
            part = got.at[o, pl.ds(0, members * rows - 2)]
            pltpu.make_async_remote_copy(
                src_ref=part, dst_ref=part, send_sem=send3, recv_sem=recv3.at[o],
                device_id=(t, m), device_id_type=MESH,
            ).wait_recv()
            unpack(o)
        place(o, lambda n, i, o=o: got[o, n * rows + i])

    shipped = got.at[pl.ds(0, members - 1), pl.ds(0, members * rows - 2)]
    pltpu.make_async_remote_copy(
        src_ref=shipped, dst_ref=shipped, send_sem=send3, recv_sem=recv3.at[0],
        device_id=(t, m), device_id_type=MESH,
    ).wait_send()
    sent = raw.at[pl.ds(0, total - 1)]
    pltpu.make_async_remote_copy(
        src_ref=sent, dst_ref=sent, send_sem=send1, recv_sem=recv1.at[0],
        device_id=(t, m), device_id_type=MESH,
    ).wait_send()


def per_device(fields):
    rows, mons, pixels = fields.shape
    tms, members = lax.axis_size("tm"), lax.axis_size("member")
    scale = 1.0 / (8.0 * float(mons * tms - 12))
    return pl.pallas_call(
        functools.partial(kernel, (tms, members, rows, mons, scale)),
        out_shape=jax.ShapeDtypeStruct((rows, rows * members, pixels // tms), F32),
        in_specs=[pl.BlockSpec(memory_space=pltpu.HBM)],
        out_specs=pl.BlockSpec(memory_space=pltpu.VMEM),
        scratch_shapes=[
            pltpu.VMEM((tms * members, rows, mons, 128), F32),
            pltpu.VMEM((members, 11, rows, 8, 128), F32),
            pltpu.VMEM((members, members, rows, rows, 128), F32),
            pltpu.VMEM((members, members * rows, rows, 128), F32),
            pltpu.SemaphoreType.DMA,
            pltpu.SemaphoreType.DMA((members,)),
            pltpu.SemaphoreType.DMA,
            pltpu.SemaphoreType.DMA,
            pltpu.SemaphoreType.DMA((members,)),
            pltpu.SemaphoreType.REGULAR,
        ],
        compiler_params=pltpu.CompilerParams(collective_id=0, has_side_effects=True, vmem_limit_bytes=50 * 2**20),
        name="cov",
    )(fields)


def solution(mesh):
    in_specs = (P("member", "tm", None),)
    out_specs = P("member", None, "tm")
    return jax.shard_map(per_device, mesh=mesh, in_specs=in_specs, out_specs=out_specs, check_vma=False)
```
